32 devices in a mesh: dp: 8 (over y, x, core), expert: 4 (over z).
Axes of the slice: x: 2, y: 2, z: 4, core: 2. Of those that a mesh axis runs over, the one named last changes fastest.
Arguments:
- tokens: bfloat16 [4096, 1792], P(('dp', 'expert')), may hold values from -6 to 6
- routes: int32 [4096, 2], P(('dp', 'expert')), may hold values from 0 to 3, all different within a row; in each aligned block of 128 rows (0 to 127, 128 to 255, ...) at most 128 rows name the same one
- gates: float32 [4096, 2], P(('dp', 'expert')), may hold values from 0.25 to 1
- grad_hidden: bfloat16 [4096, 2, 512], P(('dp', 'expert')), may hold values from -4 to 4
- w_in: bfloat16 [4, 1792, 512], P('expert', 'dp'), may hold values from -0.25 to 0.25
- error: bfloat16 [8, 4, 1792, 512], P('dp', 'expert'), may hold values from -6 to 6
- q_seed: float32 [4, 512, 32], P('expert'), may hold values from -6 to 6
Outputs:
- grad_tokens: bfloat16 [4096, 1792], P(('dp', 'expert'))
- error_next: bfloat16 [8, 4, 1792, 512], P('dp', 'expert')
- weight_grad: float32 [4, 1792, 512], P('expert', 'dp')
The draws below stay inside these ranges and needn't reach their ends.
Inputs may be any that keep to these rules, and one draw needn't show every extreme that they name: `routes`: in the rows of one device no expert is named by more than 128 rows, a bound that some block reaches; the two experts of a row differ.
All inputs are finite; a program needn't handle non-finite values.
Results may differ from the reference program's by a relative error of at most 0.014.
Values may be sent and summed in bfloat16 or wider, within the bound.
A program may use at most 64 MiB of HBM per device.

```python
import math
import jax
import jax.numpy as jnp
import numpy as np
from jax import lax

D = 1792
F = 512
RANK = 32
TOK_DEV = 128
EXPERTS = 4
REPLICAS = 8
CAP = 128
TOKENS = 4096
N_DP = 8
N_EXPERT = 4


def block_scale(own_key, dims, split, smallest, high):
    level, own = 1.0, jax.random.fold_in(own_key, 6)
    for position, blocks in split:
        draws = jnp.exp(jax.random.uniform(jax.random.fold_in(own, position), (blocks,), jnp.float32, smallest / len(split), high / len(split)))
        level = level * jnp.repeat(draws, dims[position] // blocks).reshape([-1 if axis == position else 1 for axis in range(len(dims))])
    return level


def shared_out(stream_key, own, number, rows, count, top, limit, lean):
    order = jax.random.permutation(stream_key, count)
    heavy_load, usual = portions_of(count, rows * top, limit, lean, True), portions_of(count, rows * top, limit, lean, False)
    places = jnp.arange(count)

    def named(lengths, turn):
        used = int((lengths > 0).sum())
        fixed = max(1, used // 4)
        shifted = fixed + (places - fixed + turn * (used - fixed)) % max(1, count - fixed)
        return jnp.zeros((count,), jnp.int32).at[order[jnp.where(places < fixed, places, shifted)]].set(jnp.asarray(lengths, jnp.int32))

    lengths = jnp.where(number % 4 == 0, named(heavy_load, number // 4), named(usual, number - number // 4 - 1))
    mixed = jax.random.permutation(jax.random.fold_in(own, 3), count)
    source_of, sink = mixed[0:count // 2 * 2:2], mixed[1:count // 2 * 2:2]
    slack = jnp.minimum(lengths[source_of] - 1, limit - lengths[sink]) // 2
    slack = jnp.where((source_of == order[0]) | (sink == order[0]) | (lengths[sink] == 0), 0, jnp.maximum(slack, 0))
    shifted = jax.random.randint(jax.random.fold_in(own, 4), (count // 2,), 0, 1 << 20) % (slack + 1)
    lengths = lengths.at[source_of].add(-shifted).at[sink].add(shifted)
    members = jnp.searchsorted(jnp.cumsum(lengths), jnp.arange(rows * top), side="right").astype(jnp.int32)
    listing = members.reshape(top, rows).T
    listing = listing[jax.random.permutation(jax.random.fold_in(own, 1), rows)]
    turn = jax.random.randint(jax.random.fold_in(own, 2), (rows, 1), 0, top)
    return jnp.take_along_axis(listing, (jnp.arange(top)[None, :] + turn) % top, axis=1)


def portions_of(count, total, limit, lean, full):
    weights = [(1 << 20) // math.isqrt(rank ** lean) + 1 for rank in range(1, count + 1)]
    largest = limit if full else min(limit, max(-(-total // count), total * weights[0] // sum(weights)))
    least = 1 if total - largest >= count - 1 else 0
    holding, spare = [largest] + [least] * (count - 1), total - largest - least * (count - 1)
    while spare > 0:
        movable = [i for i in range(1, count) if holding[i] < largest] or [i for i in range(1, count) if holding[i] < limit]
        mass, budget = sum([weights[i] for i in movable]), spare
        for i in movable:
            more = min(limit - holding[i], max(1, budget * weights[i] // mass), spare)
            holding[i] = holding[i] + more
            spare = spare - more
    return np.array(holding)


def gaussian(rng, extent, scale, bound, pieces=(), kind=jnp.bfloat16):
    values = jax.random.normal(rng, extent, jnp.float32) * scale
    if len(pieces) > 0:
        values = block_scale(rng, extent, pieces, -0.22, 0.18) * values
    return jnp.clip(values, min=-bound, max=bound).astype(kind)


def setup_inputs(seed: int = 0) -> dict:
    arg_keys = jax.random.split(jax.random.key(seed), 8)
    tokens = gaussian(arg_keys[0], (TOKENS, D), 1.0, 6.0, ((0, 32),))
    routes_keys = jax.random.split(jax.random.fold_in(arg_keys[1], 1), TOKENS // TOK_DEV)
    routes_turns = jax.random.permutation(jax.random.fold_in(arg_keys[1], 3), TOKENS // TOK_DEV)
    routes = jax.vmap(lambda own, number: shared_out(jax.random.fold_in(arg_keys[1], 2), own, number, TOK_DEV, EXPERTS, 2, CAP, 1))(routes_keys, routes_turns).reshape((TOKENS, 2))
    gates = jnp.clip(0.25 + 0.75 * jax.random.uniform(arg_keys[2], (TOKENS, 2), jnp.float32) ** block_scale(arg_keys[2], (TOKENS, 2), ((0, 32),), -0.2, 0.2), 0.25, 1.0)
    grad_hidden = gaussian(arg_keys[3], (TOKENS, 2, F), 0.5, 4.0, ((0, 32),))
    w_in = gaussian(arg_keys[4], (EXPERTS, D, F), F ** -0.5, 0.25, ((0, 4), (1, 8)))
    error = gaussian(arg_keys[5], (REPLICAS, EXPERTS, D, F), 1.0, 6.0, ((0, 8), (1, 4)))
    q_seed = gaussian(arg_keys[6], (EXPERTS, F, RANK), 1.0, 6.0, ((0, 4),), jnp.float32)
    return dict(tokens=tokens, routes=routes, gates=gates, grad_hidden=grad_hidden, w_in=w_in, error=error, q_seed=q_seed)


highest = lax.Precision.HIGHEST

def slopes(pre_act):
    squashed = jax.nn.sigmoid(pre_act)
    return squashed * (1.0 + pre_act * (1.0 - squashed))

def gram_schmidt(factor):
    height = factor.shape[0]

    def column(ordinal, basis):
        vector = lax.dynamic_index_in_dim(basis, ordinal, 0, keepdims=False)
        vector = vector / jnp.sqrt(jnp.sum(vector * vector))
        coeffs = jnp.dot(basis, vector, precision=highest)
        beyond = (jnp.arange(height) > ordinal).astype(basis.dtype)
        basis = basis - (coeffs * beyond)[:, None] * vector[None, :]
        return lax.dynamic_update_index_in_dim(basis, vector, ordinal, 0)
    return lax.fori_loop(0, height, column, factor)

def choose_slots(chosen, expert):
    matches = chosen == expert
    slots = jnp.cumsum(matches.astype(jnp.int32)) - 1
    target = jnp.where(matches, slots, CAP).astype(jnp.int32)
    ordinal = jnp.arange(chosen.shape[0], dtype=jnp.int32)
    indices = jnp.zeros((CAP + 1,), jnp.int32).at[target].set(ordinal)[:CAP]
    filled = jnp.zeros((CAP + 1,), jnp.float32).at[target].set(1.0)[:CAP]
    return (indices, filled)

def take_rows(source, places):
    return source[places]

def add_rows(buffer, places, values):
    return buffer.at[places].add(values)

def replica_work(arrived, arrived_grad, stored, weight):
    pre_act = jnp.dot(arrived, weight, preferred_element_type=jnp.float32)
    grad_pre = (arrived_grad.astype(jnp.float32) * slopes(pre_act)).astype(jnp.bfloat16)
    weight_term = lax.dot_general(arrived, grad_pre, (((0,), (0,)), ((), ())), preferred_element_type=jnp.float32)
    grad_rows = lax.dot_general(grad_pre, weight, (((1,), (1,)), ((), ())), preferred_element_type=jnp.float32)
    return (weight_term + stored.astype(jnp.float32), grad_rows.astype(jnp.bfloat16))

def reference(tokens, routes, gates, grad_hidden, w_in, error, q_seed):
    blocks = tokens.reshape(N_DP, N_EXPERT, TOK_DEV, D)
    chosen_all = routes.reshape(N_DP, N_EXPERT, 2 * TOK_DEV)
    gate_all = gates.reshape(N_DP, N_EXPERT, 2 * TOK_DEV)
    grad_all = grad_hidden.reshape(N_DP, N_EXPERT, 2 * TOK_DEV, F)
    slot_finder = jax.vmap(jax.vmap(choose_slots, (0, None)), (0, None))
    take_twice = jax.vmap(jax.vmap(take_rows))
    add_twice = jax.vmap(jax.vmap(add_rows))
    work_all = jax.vmap(replica_work, (0, 0, 0, None))

    def per_expert(running, expert):
        indices, filled = slot_finder(chosen_all, expert)
        token_rows = indices // 2
        gate_sel = take_twice(gate_all, indices) * filled
        scaled = (take_twice(blocks, token_rows).astype(jnp.float32) * gate_sel[..., None]).astype(jnp.bfloat16)
        sent_grad = (take_twice(grad_all, indices).astype(jnp.float32) * filled[..., None]).astype(jnp.bfloat16)
        weight = w_in[expert]
        merged, grad_rows = work_all(scaled.reshape(N_DP, N_EXPERT * CAP, D), sent_grad.reshape(N_DP, N_EXPERT * CAP, F), error[:, expert], weight)
        q_start = q_seed[expert].astype(jnp.float32)
        summed = jnp.einsum('fr,ndf->rd', q_start, merged, precision=highest) / N_DP
        basis = gram_schmidt(summed)
        q_factor = jnp.einsum('rd,ndf->rf', basis, merged, precision=highest) / N_DP
        low_rank = jnp.dot(basis.T, q_factor, precision=highest)
        error_out = (merged - low_rank[None]).astype(jnp.bfloat16)
        returned = grad_rows.reshape(N_DP, N_EXPERT, CAP, D).astype(jnp.float32) * gate_sel[..., None]
        running = add_twice(running, token_rows, returned)
        return (running, (error_out, low_rank))
    initial = jnp.zeros((N_DP, N_EXPERT, TOK_DEV, D), jnp.float32)
    running, (errors, low_rank) = lax.scan(per_expert, initial, jnp.arange(EXPERTS))
    grad_tokens = running.reshape(N_DP * N_EXPERT * TOK_DEV, D).astype(jnp.bfloat16)
    return (grad_tokens, jnp.transpose(errors, (1, 0, 2, 3)), low_rank)
```

```python
import functools

import jax
import jax.numpy as jnp
from jax import lax
from jax.experimental import pallas as pl
from jax.experimental.pallas import tpu as pltpu
from jax.sharding import PartitionSpec as P

HI = lax.Precision.HIGHEST
MESH = pl.DeviceIdType.MESH
F32 = jnp.float32
BF16 = jnp.bfloat16
NT = (((1,), (1,)), ((), ()))
TN = (((0,), (0,)), ((), ()))


def slopes(pre_act):
    squashed = 1.0 / (1.0 + jnp.exp(-pre_act))
    return squashed * (1.0 + pre_act * (1.0 - squashed))


def halves(value):
    high = value.astype(BF16)
    low = (value - high.astype(F32)).astype(BF16)
    return jnp.concatenate([high, low], axis=0)


def fold(value):
    rows = value.shape[0] // 2
    return value[:rows] + value[rows:]


def inverse_factor(gram):
    rank = gram.shape[0]
    rows = lax.broadcasted_iota(jnp.int32, (rank, rank), 0)
    cols = lax.broadcasted_iota(jnp.int32, (rank, rank), 1)
    left = gram
    right = (rows == cols).astype(F32)
    row_id = lax.broadcasted_iota(jnp.int32, (rank, 1), 0)
    for i in range(rank - 1):
        scale = 1.0 / left[i : i + 1, i : i + 1]
        col = jnp.where(row_id > i, left[:, i : i + 1], 0.0)
        row_l = left[i : i + 1, :] * scale
        row_r = right[i : i + 1, :] * scale
        left = left - col * row_l
        right = right - col * row_r
    pivots = jnp.sum(jnp.where(rows == cols, left, 0.0), axis=1, keepdims=True)
    return right * (1.0 / jnp.sqrt(pivots))


def kernel(dims, tok_hbm, gh_hbm, rt_hbm, gt_hbm, w_hbm, err_hbm, q_hbm,
           gt_out, err_out, wg_out,
           tok_all, gh_raw, gh_sel, gh_all, rt_v, gt_v, gate_sel, gate_all, w_all, x_all, gp_all,
           err_v, merged, merged_b, back, ret, q_v, q2, facc, fbuf, rsbuf, agbuf, tbuf, bt_v,
           in_s, tok_s, tok_r, gh_s, gh_r, gate_s, gate_r, w_s, w_r,
           f_s, f_r, a_s, a_r, t_s, t_r, b_s, b_r):
    E, N, rp, chunk, gather_w, C = dims
    z = lax.axis_index("expert")
    me = lax.axis_index("dp")
    tokens, width = tok_hbm.shape
    shard = width // N
    rank = q_hbm.shape[0]
    groups = width // 128
    part = tokens // C
    ready = C

    def other(axis, size, k):
        return lax.rem(lax.axis_index(axis) + k, size)

    def loop(size, fn, start=1):
        def step(k, c):
            fn(k)
            return c
        lax.fori_loop(start, size, step, 0)

    barrier = pltpu.get_barrier_semaphore()
    loop(E, lambda k: pl.semaphore_signal(
        barrier, inc=1, device_id={"expert": other("expert", E, k)}, device_id_type=MESH))
    loop(N, lambda k: pl.semaphore_signal(
        barrier, inc=1, device_id={"dp": other("dp", N, k)}, device_id_type=MESH))

    def w_rows(slot):
        return w_all.at[pl.ds(pl.multiple_of(slot * shard, 16), shard)] if gather_w else w_all

    loads = [
        pltpu.make_async_copy(tok_hbm, tok_all.at[z], in_s.at[0]),
        pltpu.make_async_copy(w_hbm, w_rows(me), in_s.at[1]),
        pltpu.make_async_copy(rt_hbm, rt_v, in_s.at[2]),
        pltpu.make_async_copy(gt_hbm, gt_v, in_s.at[3]),
        pltpu.make_async_copy(gh_hbm, gh_raw, in_s.at[4]),
        pltpu.make_async_copy(q_hbm, q_v, in_s.at[5]),
        pltpu.make_async_copy(err_hbm.at[0, 0], err_v, in_s.at[6]),
    ]
    for load in loads:
        load.start()

    def rdma(src, dst, s, r, axis, peer):
        return pltpu.make_async_remote_copy(
            src_ref=src, dst_ref=dst, send_sem=s, recv_sem=r,
            device_id={axis: peer}, device_id_type=MESH)

    def gate_copy(p, slot, k):
        return rdma(gate_sel.at[p], gate_all.at[slot], gate_s.at[k], gate_r.at[slot], "expert", p)

    def gh_copy(p, slot, k):
        return rdma(gh_sel.at[p], gh_all.at[slot], gh_s.at[k], gh_r.at[slot], "expert", p)

    def rows_of(c):
        return pl.ds(pl.multiple_of(c * part, 16), part)

    def tok_copy(j, c, nb, d):
        piece = tok_all.at[j, rows_of(c)]
        return rdma(piece, piece, tok_s.at[d, j, c], tok_r.at[j, c], "expert", nb)

    def w_copy(p, slot, k):
        return rdma(w_rows(slot), w_rows(slot), w_s.at[k], w_r.at[slot], "dp", p)

    def each(p_axis, size, copy, act):
        mine = lax.axis_index(p_axis)

        def fn(k):
            p = other(p_axis, size, k)
            if act == "start":
                copy(p, mine, k).start()
            elif act == "recv":
                copy(p, p, k).wait_recv()
            else:
                copy(p, mine, k).wait_send()
        loop(size, fn)

    partner = me + 1 - 2 * lax.rem(me, 2)
    half = N // 2

    def cross(k):
        return me + 2 * (lax.bitwise_xor(me // 2, k) - me // 2)

    for i in range(4):
        loads[i].wait()
    pl.semaphore_wait(barrier, E - 1 + N - 1)

    for d, dirn in enumerate((1, -1)):
        nb = z + dirn
        ahead = z if d == 0 else E - 1 - z

        @pl.when((nb >= 0) & (nb < E))
        def _():
            tok_copy(z, 0, nb, d).start()

            @pl.when(ahead == 0)
            def _():
                loop(C, lambda c: tok_copy(z, c, nb, d).start())
    if gather_w:
        loop(half, lambda k: w_copy(cross(k), me, k).start())
        w_copy(partner, me, 0).start()

    routes = rt_v[...]
    gates = gt_v[...]

    def pick_gate(e):
        row = jnp.where(routes[0:1] == e, gates[0:1], jnp.where(routes[1:2] == e, gates[1:2], 0.0))
        gate_sel[e] = jnp.broadcast_to(row, (8, tokens))
    loop(E, pick_gate, 0)
    each("expert", E, gate_copy, "start")
    gate_all[z] = gate_sel[z]

    loads[4].wait()
    pairs = gh_raw[...].reshape(2 * tokens, gh_raw.shape[2])
    named = jnp.transpose(jnp.concatenate([routes.astype(F32)] * 4, axis=0))
    t_id = lax.broadcasted_iota(jnp.int32, (tokens, 2 * tokens), 0)
    p_id = lax.broadcasted_iota(jnp.int32, (tokens, 2 * tokens), 1)
    wanted = jnp.where(p_id == 2 * t_id, named[:, 0:1],
                       jnp.where(p_id == 2 * t_id + 1, named[:, 1:2], -1.0))

    def pick_rows(e):
        choose = jnp.where(wanted == e.astype(F32), 1.0, 0.0).astype(BF16)
        gh_sel[e] = jnp.dot(choose, pairs, preferred_element_type=F32).astype(BF16)

    def send_rows(k):
        p = other("expert", E, k)
        pick_rows(p)
        gh_copy(p, z, k).start()
    loop(E, send_rows)
    pick_rows(z)
    gh_all[z] = gh_sel[z]

    loads[5].wait()
    loads[6].wait()
    q2[...] = halves(q_v[...])

    def err_factor(c):
        cols = pl.ds(pl.multiple_of(c * chunk, chunk), chunk)
        facc[:, cols] = fold(lax.dot_general(
            q2[...], err_v[cols, :], NT, preferred_element_type=F32))
    loop(width // chunk, err_factor, 0)

    def back_copy(dest, c):
        dirn = jnp.where(dest > z, 1, -1)
        nb = z + dirn
        slot = jnp.where((dest == nb) & (dest < z), E, dest)
        return rdma(back.at[dest, rows_of(c)], ret.at[slot, rows_of(c)],
                    b_s.at[dest, c], b_r.at[slot, c], "expert", nb)

    def back_wait(slot, c):
        rdma(back.at[0, rows_of(c)], ret.at[slot, rows_of(c)], b_s.at[0, c], b_r.at[slot, c],
             "expert", other("expert", E, 1)).wait_recv()

    def add_back(dest, slot, c):
        rows = rows_of(c)
        back[dest, rows, :] = (back[dest, rows, :].astype(F32)
                               + ret[slot, rows, :].astype(F32)).astype(BF16)

    def compute(j):
        @pl.when(j != z)
        def _():
            gate_copy(j, j, 0).wait_recv()
            gh_copy(j, j, 0).wait_recv()
        g = jnp.transpose(gate_all[j])[:, :1]
        x = (tok_all[j].astype(F32) * g).astype(BF16)
        x_all[j] = x
        pre = jnp.dot(x, w_all[...], preferred_element_type=F32)
        gp = (gh_all[j].astype(F32) * slopes(pre)).astype(BF16)
        gp_all[j] = gp
        seen = fold(lax.dot_general(q2[...], gp, NT, preferred_element_type=F32))
        facc[...] += fold(jnp.dot(halves(seen), x, preferred_element_type=F32))
        back[j] = (lax.dot_general(gp, w_all[...], NT, preferred_element_type=F32) * g).astype(BF16)

        @pl.when(((j > z) & (z == 0)) | ((j < z) & (z == E - 1)))
        def _():
            loop(C, lambda c: back_copy(j, c).start(), 0)

    def stage(e, ahead):
        early = e < ahead
        rest = jnp.maximum(e - ahead, 0)
        s = jnp.where(early, e + 1, ahead - rest // (C - 1))
        c = jnp.where(early, 0, lax.rem(rest, C - 1) + 1)
        return s, c, e < ahead * C

    def event(e):
        for d, dirn in enumerate((1, -1)):
            ahead = z if d == 0 else E - 1 - z
            s, c, valid = stage(e, ahead)
            j = z - dirn * s
            nb = z + dirn
            linked = (nb >= 0) & (nb < E)

            @pl.when(valid)
            def _():
                tok_copy(j, c, z, d).wait_recv()

                @pl.when(linked)
                def _():
                    tok_copy(j, c, nb, d).start()

                    @pl.when(e == ahead * C - 1)
                    def _():
                        loop(C, lambda k: tok_copy(z, k, nb, d).start())
        if gather_w:
            @pl.when(e == 2)
            def _():
                def forward(k):
                    w_copy(cross(k), cross(k), 0).wait_recv()
                    w_copy(partner, cross(k), half + k).start()
                loop(min(3, half), forward)

            @pl.when(e == ready)
            def _():
                def forward(k):
                    w_copy(cross(k), cross(k), 0).wait_recv()
                    w_copy(partner, cross(k), half + k).start()
                loop(half, forward, min(3, half))
                w_copy(partner, partner, 0).wait_recv()
                loop(half, lambda k: w_copy(partner, partner + cross(k) - me, 0).wait_recv())

        def slot(i, carry):
            ahead = jnp.where(i == 0, z, E - 1 - z)
            dirn = 1 - 2 * i
            s, c, valid = stage(e, ahead)
            first = ahead + C - 2
            late = (e == ready) & (first < ready) & (ahead > 0)
            done = (e >= ready) & valid & (c == C - 1)
            own = (i == 2) & (e == ready + 2)
            j = jnp.where(own, z, jnp.where(late, z - dirn * ahead, z - dirn * s))

            @pl.when(own | ((i < 2) & (late | done)))
            def _():
                compute(j)
            return carry

        @pl.when(e >= ready)
        def _():
            lax.fori_loop(0, 3, slot, 0)
    loop((E - 1) * C, event, 0)

    if fbuf.shape[0] > groups * rank:
        fbuf[...] = jnp.zeros_like(fbuf)
    for c in range(groups):
        fbuf[c * rank : (c + 1) * rank, :] = facc[:, c * 128 : (c + 1) * 128]

    def f_copy(p, slot, k):
        return rdma(fbuf.at[pl.ds(pl.multiple_of(p * rp, 8), rp)], rsbuf.at[slot],
                    f_s.at[k], f_r.at[slot], "dp", p)

    def a_copy(p, slot, k):
        piece = agbuf.at[pl.ds(pl.multiple_of(slot * rp, 8), rp)]
        return rdma(piece, piece, a_s.at[k], a_r.at[slot], "dp", p)

    def t_copy(p, slot, k):
        return rdma(tbuf.at[slot], tbuf.at[slot], t_s.at[k], t_r.at[slot], "dp", p)

    own = pl.ds(pl.multiple_of(me * rp, 8), rp)
    each("dp", N, f_copy, "start")
    rsbuf[me] = fbuf[own, :]

    def merge(c):
        cols = pl.ds(pl.multiple_of(c * chunk, chunk), chunk)
        x = x_all[:, :, cols].reshape(E * tokens, chunk)
        gp = gp_all[...].reshape(E * tokens, gp_all.shape[2])
        m = lax.dot_general(x, gp, TN, preferred_element_type=F32)
        m = m + err_v[cols, :].astype(F32)
        merged[cols, :] = m
        merged_b[cols, :] = m.astype(BF16)
    loop(width // chunk, merge, 0)

    each("dp", N, f_copy, "recv")
    agbuf[own, :] = jnp.sum(rsbuf[...], axis=0) * (1.0 / N)
    each("dp", N, a_copy, "start")

    right_first = z < E - 1 - z

    def relay(dest):
        def piece(c):
            back_wait(dest, c)
            add_back(dest, dest, c)
            back_copy(dest, c).start()
        loop(C, piece, 0)

    def relay_right(k):
        dest = E - k

        @pl.when((dest > z) & (z > 0))
        def _():
            relay(dest)

    def relay_left(k):
        dest = k - 1

        @pl.when((dest < z) & (z < E - 1))
        def _():
            relay(dest)

    @pl.when(right_first)
    def _():
        loop(E, relay_right)

    @pl.when(jnp.logical_not(right_first))
    def _():
        loop(E, relay_left)

    each("dp", N, a_copy, "recv")
    factor = jnp.concatenate([agbuf[c * rank : (c + 1) * rank, :] for c in range(groups)], axis=1)
    tbuf[me] = fold(jnp.dot(halves(factor), merged_b[...], preferred_element_type=F32)).astype(BF16)
    each("dp", N, t_copy, "start")

    gram = lax.dot_general(factor, factor, NT, precision=HI, preferred_element_type=F32)
    inverse = inverse_factor(gram)
    basis = jnp.dot(inverse, factor, precision=HI, preferred_element_type=F32)
    bt_v[...] = jnp.transpose(basis).astype(BF16)

    @pl.when(right_first)
    def _():
        loop(E, relay_left)

    @pl.when(jnp.logical_not(right_first))
    def _():
        loop(E, relay_right)

    each("dp", N, t_copy, "recv")
    mean = jnp.sum(tbuf[...].astype(F32), axis=0) * (1.0 / N)
    q_factor = jnp.dot(inverse, mean, precision=HI, preferred_element_type=F32).astype(BF16)

    for c in range(width // chunk):
        cols = pl.ds(c * chunk, chunk)
        low = jnp.dot(bt_v[cols, :], q_factor, preferred_element_type=F32)
        err_out[0, 0, cols, :] = (merged[cols, :] - low).astype(BF16)
    wg_out[0] = jnp.dot(bt_v[pl.ds(pl.multiple_of(me * shard, 8), shard), :], q_factor,
                        preferred_element_type=F32)

    @pl.when(z > 0)
    def _():
        def piece(c):
            back_wait(z, c)
            add_back(z, z, c)
        loop(C, piece, 0)

    @pl.when(z < E - 1)
    def _():
        def piece(c):
            back_wait(E, c)
            add_back(z, E, c)
        loop(C, piece, 0)
    gt_out[...] = back[z]

    for d, dirn in enumerate((1, -1)):
        nb = z + dirn
        ahead = z if d == 0 else E - 1 - z

        @pl.when((nb >= 0) & (nb < E))
        def _():
            def drain(s):
                @pl.when(s <= ahead)
                def _():
                    loop(C, lambda c: tok_copy(z - dirn * s, c, nb, d).wait_send(), 0)
            loop(E, drain, 0)
    each("expert", E, gate_copy, "send")
    each("expert", E, gh_copy, "send")
    if gather_w:
        loop(half, lambda k: w_copy(cross(k), me, k).wait_send())
        w_copy(partner, me, 0).wait_send()
        loop(half, lambda k: w_copy(partner, cross(k), half + k).wait_send())

    def sent(k):
        dest = other("expert", E, k)
        loop(C, lambda c: back_copy(dest, c).wait_send(), 0)
    loop(E, sent)
    each("dp", N, f_copy, "send")
    each("dp", N, a_copy, "send")
    each("dp", N, t_copy, "send")


def body(tokens, routes, gates, grad_hidden, w_in, error, q_seed):
    E = lax.axis_size("expert")
    N = lax.axis_size("dp")
    rows, width = tokens.shape
    hidden = grad_hidden.shape[2]
    rank = q_seed.shape[2]
    shard = width // N
    gather_w = shard % 16 == 0 and N & (N - 1) == 0
    weight = w_in[0] if gather_w else lax.all_gather(w_in[0], "dp", axis=0, tiled=True)
    chunk = 256 if width % 256 == 0 else 128
    C = 4 if E <= 8 else 2
    total_rows = width // 128 * rank
    rp = -(-total_rows // N)
    rp = -(-rp // 8) * 8
    dma = pltpu.SemaphoreType.DMA
    vmem = pl.BlockSpec(memory_space=pltpu.VMEM)
    hbm = pl.BlockSpec(memory_space=pltpu.HBM)
    return pl.pallas_call(
        functools.partial(kernel, (E, N, rp, chunk, gather_w, C)),
        out_shape=(
            jax.ShapeDtypeStruct((rows, width), BF16),
            jax.ShapeDtypeStruct((1, 1, width, hidden), BF16),
            jax.ShapeDtypeStruct((1, shard, hidden), F32),
        ),
        in_specs=[hbm] * 7,
        out_specs=(vmem, vmem, vmem),
        scratch_shapes=[
            pltpu.VMEM((E, rows, width), BF16),
            pltpu.VMEM((rows, 2, hidden), BF16),
            pltpu.VMEM((E, rows, hidden), BF16),
            pltpu.VMEM((E, rows, hidden), BF16),
            pltpu.VMEM((2, rows), jnp.int32),
            pltpu.VMEM((2, rows), F32),
            pltpu.VMEM((E, 8, rows), F32),
            pltpu.VMEM((E, 8, rows), F32),
            pltpu.VMEM((width, hidden), BF16),
            pltpu.VMEM((E, rows, width), BF16),
            pltpu.VMEM((E, rows, hidden), BF16),
            pltpu.VMEM((width, hidden), BF16),
            pltpu.VMEM((width, hidden), F32),
            pltpu.VMEM((width, hidden), BF16),
            pltpu.VMEM((E, rows, width), BF16),
            pltpu.VMEM((E + 1, rows, width), BF16),
            pltpu.VMEM((rank, hidden), F32),
            pltpu.VMEM((2 * rank, hidden), BF16),
            pltpu.VMEM((rank, width), F32),
            pltpu.VMEM((rp * N, 128), F32),
            pltpu.VMEM((N, rp, 128), F32),
            pltpu.VMEM((rp * N, 128), F32),
            pltpu.VMEM((N, rank, hidden), BF16),
            pltpu.VMEM((width, rank), BF16),
            dma((7,)), dma((2, E, C)), dma((E, C)), dma((E,)), dma((E,)), dma((E,)), dma((E,)),
            dma((N,)), dma((N,)), dma((N,)), dma((N,)), dma((N,)), dma((N,)), dma((N,)), dma((N,)),
            dma((E, C)), dma((E + 1, C)),
        ],
        compiler_params=pltpu.CompilerParams(
            collective_id=0, has_side_effects=True, vmem_limit_bytes=67043328 - (1 << 20)),
    )(tokens, grad_hidden, routes.T, gates.T, weight, error, q_seed[0].T)


def solution(mesh):
    placed = (
        P(("dp", "expert"), None),
        P(("dp", "expert"), None),
        P(("dp", "expert"), None),
        P(("dp", "expert"), None, None),
        P("expert", "dp", None),
        P("dp", "expert", None, None),
        P("expert", None, None),
    )
    return jax.shard_map(
        body,
        mesh=mesh,
        in_specs=placed,
        out_specs=(
            P(("dp", "expert"), None),
            P("dp", "expert", None, None),
            P("expert", "dp", None),
        ),
        check_vma=False,
    )
```

```python
import functools

import jax
import jax.numpy as jnp
from jax import lax
from jax.experimental import pallas as pl
from jax.experimental.pallas import tpu as pltpu
from jax.sharding import PartitionSpec as P

HI = lax.Precision.HIGHEST
MESH = pl.DeviceIdType.MESH
F32 = jnp.float32
BF16 = jnp.bfloat16
NT = (((1,), (1,)), ((), ()))
TN = (((0,), (0,)), ((), ()))


def slopes(pre_act):
    squashed = 1.0 / (1.0 + jnp.exp(-pre_act))
    return squashed * (1.0 + pre_act * (1.0 - squashed))


def halves(value):
    high = value.astype(BF16)
    low = (value - high.astype(F32)).astype(BF16)
    return jnp.concatenate([high, low], axis=0)


def fold(value):
    rows = value.shape[0] // 2
    return value[:rows] + value[rows:]


def inverse_factor(gram):
    rank = gram.shape[0]
    rows = lax.broadcasted_iota(jnp.int32, (rank, rank), 0)
    cols = lax.broadcasted_iota(jnp.int32, (rank, rank), 1)
    left = gram
    right = (rows == cols).astype(F32)
    row_id = lax.broadcasted_iota(jnp.int32, (rank, 1), 0)
    for i in range(rank - 1):
        scale = 1.0 / left[i : i + 1, i : i + 1]
        col = jnp.where(row_id > i, left[:, i : i + 1], 0.0)
        row_l = left[i : i + 1, :] * scale
        row_r = right[i : i + 1, :] * scale
        left = left - col * row_l
        right = right - col * row_r
    pivots = jnp.sum(jnp.where(rows == cols, left, 0.0), axis=1, keepdims=True)
    return right * (1.0 / jnp.sqrt(pivots))


def kernel(dims, tok_hbm, gh_hbm, rt_hbm, gt_hbm, w_hbm, err_hbm, q_hbm,
           gt_out, err_out, wg_out,
           tok_all, gh_raw, gh_sel, gh_all, rt_v, gt_v, gate_sel, gate_all, w_all, x_all, gp_all,
           err_v, merged, merged_b, back, ret, q_v, q2, facc, fbuf, rsbuf, agbuf, tbuf, bt_v,
           in_s, tok_s, tok_r, gh_s, gh_r, gate_s, gate_r, w_s, w_r,
           f_s, f_r, a_s, a_r, t_s, t_r, b_s, b_r):
    E, N, rp, chunk, gather_w, C, CB = dims
    z = lax.axis_index("expert")
    me = lax.axis_index("dp")
    tokens, width = tok_hbm.shape
    shard = width // N
    rank = q_hbm.shape[0]
    groups = width // 128
    part = tokens // C
    back_part = tokens // CB

    def other(axis, size, k):
        return lax.rem(lax.axis_index(axis) + k, size)

    def loop(size, fn, start=1):
        def step(k, c):
            fn(k)
            return c
        lax.fori_loop(start, size, step, 0)

    barrier = pltpu.get_barrier_semaphore()
    loop(E, lambda k: pl.semaphore_signal(
        barrier, inc=1, device_id={"expert": other("expert", E, k)}, device_id_type=MESH))
    loop(N, lambda k: pl.semaphore_signal(
        barrier, inc=1, device_id={"dp": other("dp", N, k)}, device_id_type=MESH))

    def w_rows(slot):
        return w_all.at[pl.ds(pl.multiple_of(slot * shard, 16), shard)] if gather_w else w_all

    loads = [
        pltpu.make_async_copy(tok_hbm, tok_all.at[z], in_s.at[0]),
        pltpu.make_async_copy(w_hbm, w_rows(me), in_s.at[1]),
        pltpu.make_async_copy(rt_hbm, rt_v, in_s.at[2]),
        pltpu.make_async_copy(gt_hbm, gt_v, in_s.at[3]),
        pltpu.make_async_copy(gh_hbm, gh_raw, in_s.at[4]),
        pltpu.make_async_copy(q_hbm, q_v, in_s.at[5]),
        pltpu.make_async_copy(err_hbm.at[0, 0], err_v, in_s.at[6]),
    ]
    for load in loads:
        load.start()

    def rdma(src, dst, s, r, axis, peer):
        return pltpu.make_async_remote_copy(
            src_ref=src, dst_ref=dst, send_sem=s, recv_sem=r,
            device_id={axis: peer}, device_id_type=MESH)

    def gate_copy(p, slot, k):
        return rdma(gate_sel.at[p], gate_all.at[slot], gate_s.at[k], gate_r.at[slot], "expert", p)

    def gh_copy(p, slot, k):
        return rdma(gh_sel.at[p], gh_all.at[slot], gh_s.at[k], gh_r.at[slot], "expert", p)

    def rows_of(c):
        return pl.ds(pl.multiple_of(c * part, 16), part)

    def tok_copy(j, c, nb, d):
        piece = tok_all.at[j, rows_of(c)]
        return rdma(piece, piece, tok_s.at[d, j, c], tok_r.at[j, c], "expert", nb)

    def w_copy(p, slot, k):
        return rdma(w_rows(slot), w_rows(slot), w_s.at[k], w_r.at[slot], "dp", p)

    def each(p_axis, size, copy, act):
        mine = lax.axis_index(p_axis)

        def fn(k):
            p = other(p_axis, size, k)
            if act == "start":
                copy(p, mine, k).start()
            elif act == "recv":
                copy(p, p, k).wait_recv()
            else:
                copy(p, mine, k).wait_send()
        loop(size, fn)

    partner = me + 1 - 2 * lax.rem(me, 2)
    half = N // 2

    def cross(k):
        return me + 2 * (lax.bitwise_xor(me // 2, k) - me // 2)

    for i in range(4):
        loads[i].wait()
    pl.semaphore_wait(barrier, E - 1 + N - 1)

    for d, dirn in enumerate((1, -1)):
        nb = z + dirn

        @pl.when((nb >= 0) & (nb < E))
        def _():
            loop(C, lambda c: tok_copy(z, c, nb, d).start(), 0)
    if gather_w:
        loop(half, lambda k: w_copy(cross(k), me, k).start())
        w_copy(partner, me, 0).start()

    routes = rt_v[...]
    gates = gt_v[...]

    def pick_gate(e):
        row = jnp.where(routes[0:1] == e, gates[0:1], jnp.where(routes[1:2] == e, gates[1:2], 0.0))
        gate_sel[e] = jnp.broadcast_to(row, (8, tokens))
    loop(E, pick_gate, 0)
    each("expert", E, gate_copy, "start")
    gate_all[z] = gate_sel[z]

    loads[4].wait()
    pairs = gh_raw[...].reshape(2 * tokens, gh_raw.shape[2])
    named = jnp.transpose(jnp.concatenate([routes.astype(F32)] * 4, axis=0))
    t_id = lax.broadcasted_iota(jnp.int32, (tokens, 2 * tokens), 0)
    p_id = lax.broadcasted_iota(jnp.int32, (tokens, 2 * tokens), 1)
    wanted = jnp.where(p_id == 2 * t_id, named[:, 0:1],
                       jnp.where(p_id == 2 * t_id + 1, named[:, 1:2], -1.0))

    def pick_rows(e):
        choose = jnp.where(wanted == e.astype(F32), 1.0, 0.0).astype(BF16)
        gh_sel[e] = jnp.dot(choose, pairs, preferred_element_type=F32).astype(BF16)

    def send_rows(k):
        p = other("expert", E, k)
        pick_rows(p)
        gh_copy(p, z, k).start()
    loop(E, send_rows)
    pick_rows(z)
    gh_all[z] = gh_sel[z]

    loads[5].wait()
    loads[6].wait()
    q2[...] = halves(q_v[...])

    def err_factor(c):
        cols = pl.ds(pl.multiple_of(c * chunk, chunk), chunk)
        facc[:, cols] = fold(lax.dot_general(
            q2[...], err_v[cols, :], NT, preferred_element_type=F32))
    loop(width // chunk, err_factor, 0)

    def back_rows(c):
        return pl.ds(pl.multiple_of(c * back_part, 16), back_part)

    def back_copy(dest, c):
        dirn = jnp.where(dest > z, 1, -1)
        nb = z + dirn
        slot = jnp.where((dest == nb) & (dest < z), E, dest)
        return rdma(back.at[dest, back_rows(c)], ret.at[slot, back_rows(c)],
                    b_s.at[dest, c], b_r.at[slot, c], "expert", nb)

    def back_wait(slot, c):
        rdma(back.at[0, back_rows(c)], ret.at[slot, back_rows(c)], b_s.at[0, c], b_r.at[slot, c],
             "expert", other("expert", E, 1)).wait_recv()

    def add_back(dest, slot, c):
        rows = back_rows(c)
        back[dest, rows, :] = (back[dest, rows, :].astype(F32)
                               + ret[slot, rows, :].astype(F32)).astype(BF16)

    def gate_column(j):
        return jnp.transpose(gate_all[j])[:, :1]

    def inward(j):
        @pl.when(j != z)
        def _():
            gate_copy(j, j, 0).wait_recv()
            gh_copy(j, j, 0).wait_recv()
        x = (tok_all[j].astype(F32) * gate_column(j)).astype(BF16)
        x_all[j] = x
        pre = jnp.dot(x, w_all[...], preferred_element_type=F32)
        gp = (gh_all[j].astype(F32) * slopes(pre)).astype(BF16)
        gp_all[j] = gp
        seen = fold(lax.dot_general(q2[...], gp, NT, preferred_element_type=F32))
        facc[...] += fold(jnp.dot(halves(seen), x, preferred_element_type=F32))

    def outward(j):
        back[j] = (lax.dot_general(gp_all[j], w_all[...], NT, preferred_element_type=F32)
                   * gate_column(j)).astype(BF16)

        @pl.when(((j > z) & (z == 0)) | ((j < z) & (z == E - 1)))
        def _():
            loop(CB, lambda c: back_copy(j, c).start(), 0)

    def forward(s):
        def piece(c):
            for d, dirn in enumerate((1, -1)):
                j = z - dirn * s
                nb = z + dirn

                @pl.when((j >= 0) & (j < E))
                def _():
                    tok_copy(j, c, z, d).wait_recv()

                    @pl.when((nb >= 0) & (nb < E))
                    def _():
                        tok_copy(j, c, nb, d).start()
        loop(C, piece, 0)

    def weights():
        def pass_on(k):
            w_copy(cross(k), cross(k), 0).wait_recv()
            w_copy(partner, cross(k), half + k).start()
        loop(half, pass_on)
        w_copy(partner, partner, 0).wait_recv()
        loop(half, lambda k: w_copy(partner, partner + cross(k) - me, 0).wait_recv())

    farthest = jnp.maximum(z, E - 1 - z)

    def step(s):
        forward(s)
        if gather_w:
            @pl.when(s == 1)
            def _():
                weights()

        def block(i, carry):
            j = jnp.where(i == 0, z, jnp.where(i == 1, z - s, z + s))

            @pl.when((j >= 0) & (j < E) & ((i > 0) | (s == 1)))
            def _():
                inward(j)

                @pl.when((s < farthest) | (i == 0))
                def _():
                    outward(j)
            return carry
        lax.fori_loop(0, 3, block, 0)
    loop(E, step)

    if fbuf.shape[0] > groups * rank:
        fbuf[...] = jnp.zeros_like(fbuf)
    for c in range(groups):
        fbuf[c * rank : (c + 1) * rank, :] = facc[:, c * 128 : (c + 1) * 128]

    def f_copy(p, slot, k):
        return rdma(fbuf.at[pl.ds(pl.multiple_of(p * rp, 8), rp)], rsbuf.at[slot],
                    f_s.at[k], f_r.at[slot], "dp", p)

    def a_copy(p, slot, k):
        piece = agbuf.at[pl.ds(pl.multiple_of(slot * rp, 8), rp)]
        return rdma(piece, piece, a_s.at[k], a_r.at[slot], "dp", p)

    def t_copy(p, slot, k):
        return rdma(tbuf.at[slot], tbuf.at[slot], t_s.at[k], t_r.at[slot], "dp", p)

    own = pl.ds(pl.multiple_of(me * rp, 8), rp)
    each("dp", N, f_copy, "start")
    rsbuf[me] = fbuf[own, :]

    def last_block(i, carry):
        j = jnp.where(i == 0, z - farthest, z + farthest)

        @pl.when((j >= 0) & (j < E))
        def _():
            outward(j)
        return carry
    lax.fori_loop(0, 2, last_block, 0)

    right_first = z < E - 1 - z
    lag = 3

    def relay(m, c):
        def turn(i, carry):
            right = (i == 0) == right_first
            dest = jnp.where(right, m, E - 1 - m)
            hop = jnp.where(right, (dest > z) & (z > 0), (dest < z) & (z < E - 1))
            piece = c - lag * i

            @pl.when(hop & (piece >= 0) & (piece < CB))
            def _():
                back_wait(dest, piece)
                add_back(dest, dest, piece)
                back_copy(dest, piece).start()
            return carry
        lax.fori_loop(0, 2, turn, 0)

    def relays(start, stop, first, last):
        def rank_of(m, carry):
            loop(last, lambda c: relay(m, c), first)
            return carry
        lax.fori_loop(start, stop, rank_of, 0)

    def merge(c):
        cols = pl.ds(pl.multiple_of(c * chunk, chunk), chunk)
        x = x_all[:, :, cols].reshape(E * tokens, chunk)
        gp = gp_all[...].reshape(E * tokens, gp_all.shape[2])
        m = lax.dot_general(x, gp, TN, preferred_element_type=F32)
        m = m + err_v[cols, :].astype(F32)
        merged[cols, :] = m
        merged_b[cols, :] = m.astype(BF16)
    loop(width // chunk, merge, 0)
    relays(1, E - 1, 0, CB // 2)
    each("dp", N, f_copy, "recv")
    agbuf[own, :] = jnp.sum(rsbuf[...], axis=0) * (1.0 / N)
    each("dp", N, a_copy, "start")

    relays(1, E - 1, CB // 2, CB + lag)
    each("dp", N, a_copy, "recv")
    factor = jnp.concatenate([agbuf[c * rank : (c + 1) * rank, :] for c in range(groups)], axis=1)
    tbuf[me] = fold(jnp.dot(halves(factor), merged_b[...], preferred_element_type=F32)).astype(BF16)
    each("dp", N, t_copy, "start")

    gram = lax.dot_general(factor, factor, NT, precision=HI, preferred_element_type=F32)
    inverse = inverse_factor(gram)
    basis = jnp.dot(inverse, factor, precision=HI, preferred_element_type=F32)
    bt_v[...] = jnp.transpose(basis).astype(BF16)

    relays(E - 1, E, 0, CB + lag)
    for d, dirn in enumerate((1, -1)):
        nb = z + dirn
        ahead = z if d == 0 else E - 1 - z

        @pl.when((nb >= 0) & (nb < E))
        def _():
            def drain(s):
                @pl.when(s <= ahead)
                def _():
                    loop(C, lambda c: tok_copy(z - dirn * s, c, nb, d).wait_send(), 0)
            loop(E, drain, 0)
    each("expert", E, gate_copy, "send")
    each("expert", E, gh_copy, "send")
    if gather_w:
        loop(half, lambda k: w_copy(cross(k), me, k).wait_send())
        w_copy(partner, me, 0).wait_send()
        loop(half, lambda k: w_copy(partner, cross(k), half + k).wait_send())
    each("dp", N, f_copy, "send")
    each("dp", N, a_copy, "send")
    each("dp", N, t_copy, "recv")
    mean = jnp.sum(tbuf[...].astype(F32), axis=0) * (1.0 / N)
    q_factor = jnp.dot(inverse, mean, precision=HI, preferred_element_type=F32).astype(BF16)

    for c in range(width // chunk):
        cols = pl.ds(c * chunk, chunk)
        low = jnp.dot(bt_v[cols, :], q_factor, preferred_element_type=F32)
        err_out[0, 0, cols, :] = (merged[cols, :] - low).astype(BF16)
    wg_out[0] = jnp.dot(bt_v[pl.ds(pl.multiple_of(me * shard, 8), shard), :], q_factor,
                        preferred_element_type=F32)

    @pl.when(z > 0)
    def _():
        def piece(c):
            back_wait(z, c)
            add_back(z, z, c)
        loop(CB, piece, 0)

    @pl.when(z < E - 1)
    def _():
        def piece(c):
            back_wait(E, c)
            add_back(z, E, c)
        loop(CB, piece, 0)
    gt_out[...] = back[z]

    def sent(k):
        dest = other("expert", E, k)
        loop(CB, lambda c: back_copy(dest, c).wait_send(), 0)
    loop(E, sent)
    each("dp", N, t_copy, "send")


def body(tokens, routes, gates, grad_hidden, w_in, error, q_seed):
    E = lax.axis_size("expert")
    N = lax.axis_size("dp")
    rows, width = tokens.shape
    hidden = grad_hidden.shape[2]
    rank = q_seed.shape[2]
    shard = width // N
    gather_w = shard % 16 == 0 and N & (N - 1) == 0
    weight = w_in[0] if gather_w else lax.all_gather(w_in[0], "dp", axis=0, tiled=True)
    chunk = 256 if width % 256 == 0 else 128
    C, CB = (4, 8) if E <= 8 else (2, 2)
    room = (4 * E + 3) * rows * width * 2 + 3 * E * rows * hidden * 2 + 13 * width * hidden + (12 << 20)
    total_rows = width // 128 * rank
    rp = -(-total_rows // N)
    rp = -(-rp // 8) * 8
    dma = pltpu.SemaphoreType.DMA
    vmem = pl.BlockSpec(memory_space=pltpu.VMEM)
    hbm = pl.BlockSpec(memory_space=pltpu.HBM)
    return pl.pallas_call(
        functools.partial(kernel, (E, N, rp, chunk, gather_w, C, CB)),
        out_shape=(
            jax.ShapeDtypeStruct((rows, width), BF16),
            jax.ShapeDtypeStruct((1, 1, width, hidden), BF16),
            jax.ShapeDtypeStruct((1, shard, hidden), F32),
        ),
        in_specs=[hbm] * 7,
        out_specs=(vmem, vmem, vmem),
        scratch_shapes=[
            pltpu.VMEM((E, rows, width), BF16),
            pltpu.VMEM((rows, 2, hidden), BF16),
            pltpu.VMEM((E, rows, hidden), BF16),
            pltpu.VMEM((E, rows, hidden), BF16),
            pltpu.VMEM((2, rows), jnp.int32),
            pltpu.VMEM((2, rows), F32),
            pltpu.VMEM((E, 8, rows), F32),
            pltpu.VMEM((E, 8, rows), F32),
            pltpu.VMEM((width, hidden), BF16),
            pltpu.VMEM((E, rows, width), BF16),
            pltpu.VMEM((E, rows, hidden), BF16),
            pltpu.VMEM((width, hidden), BF16),
            pltpu.VMEM((width, hidden), F32),
            pltpu.VMEM((width, hidden), BF16),
            pltpu.VMEM((E, rows, width), BF16),
            pltpu.VMEM((E + 1, rows, width), BF16),
            pltpu.VMEM((rank, hidden), F32),
            pltpu.VMEM((2 * rank, hidden), BF16),
            pltpu.VMEM((rank, width), F32),
            pltpu.VMEM((rp * N, 128), F32),
            pltpu.VMEM((N, rp, 128), F32),
            pltpu.VMEM((rp * N, 128), F32),
            pltpu.VMEM((N, rank, hidden), BF16),
            pltpu.VMEM((width, rank), BF16),
            dma((7,)), dma((2, E, C)), dma((E, C)), dma((E,)), dma((E,)), dma((E,)), dma((E,)),
            dma((N,)), dma((N,)), dma((N,)), dma((N,)), dma((N,)), dma((N,)), dma((N,)), dma((N,)),
            dma((E, CB)), dma((E + 1, CB)),
        ],
        compiler_params=pltpu.CompilerParams(
            collective_id=0, has_side_effects=True, vmem_limit_bytes=min(room, 67043328 - (1 << 20))),
    )(*(pltpu.with_memory_space_constraint(a, pltpu.HBM) for a in (
        tokens, grad_hidden, routes.T, gates.T, weight, error, q_seed[0].T)))


def solution(mesh):
    placed = (
        P(("dp", "expert"), None),
        P(("dp", "expert"), None),
        P(("dp", "expert"), None),
        P(("dp", "expert"), None, None),
        P("expert", "dp", None),
        P("dp", "expert", None, None),
        P("expert", None, None),
    )
    return jax.shard_map(
        body,
        mesh=mesh,
        in_specs=placed,
        out_specs=(
            P(("dp", "expert"), None),
            P("dp", "expert", None, None),
            P("expert", "dp", None),
        ),
        check_vma=False,
    )
```

```python
import functools

import jax
import jax.numpy as jnp
from jax import lax
from jax.experimental import pallas as pl
from jax.experimental.pallas import tpu as pltpu
from jax.sharding import PartitionSpec as P

HI = lax.Precision.HIGHEST
MESH = pl.DeviceIdType.MESH
F32 = jnp.float32
BF16 = jnp.bfloat16
NT = (((1,), (1,)), ((), ()))
TN = (((0,), (0,)), ((), ()))


PLAN = (
    (
        (("g", 1), ("g", 2), ("g", 3),),
        (("w", 1, 0), ("w", 1, 1), ("w", 1, 2), ("w", 1, 3), ("W",), ("u", 1, 0, 1),),
        (("u", 1, 1, 0),),
        (("w", 2, 0), ("w", 2, 1), ("u", 0, 0, 1),),
        (("u", 0, 1, 0),),
        (("u", 2, 0, 1),),
        (("w", 3, 0), ("w", 3, 1), ("u", 3, 0, 1),),
        (("w", 3, 2), ("w", 3, 3), ("u", 3, 1, 0),),
        (("w", 2, 2), ("w", 2, 3), ("u", 2, 1, 0),),
    ),
    (
        (("g", 0), ("g", 2), ("g", 3),),
        (("w", 0, 0), ("r", 1, 0, 0), ("w", 2, 0), ("r", -1, 2, 0), ("w", 0, 1), ("r", 1, 0, 1), ("w", 2, 1), ("r", -1, 2, 1), ("w", 0, 2), ("r", 1, 0, 2), ("w", 2, 2), ("w", 0, 3), ("r", 1, 0, 3), ("w", 2, 3), ("W",), ("u", 1, 0, 1),),
        (("u", 1, 1, 0),),
        (("u", 0, 0, 1),),
        (("u", 0, 1, 0),),
        (("u", 2, 0, 1),),
        (("u", 2, 1, 0),),
        (("w", 3, 0), ("r", -1, 3, 0), ("w", 3, 1), ("r", -1, 3, 1), ("u", 3, 0, 1),),
        (("w", 3, 2), ("r", -1, 3, 2), ("w", 3, 3), ("r", -1, 3, 3), ("r", -1, 2, 2), ("r", -1, 2, 3), ("u", 3, 1, 0),),
    ),
)
RELAYS = (
    (2, 0), (2, 1), (2, 2), (2, 3), (3, 0), (3, 1), (3, 2), (3, 3),
    (0, 0), (3, 4), (0, 1), (3, 5), (0, 2), (3, 6), (0, 3), (3, 7),
    (0, 4), (0, 5), (0, 6), (0, 7), (2, 4), (2, 5), (2, 6), (2, 7),
)
STOPS = (4, 6, 8)


def slopes(pre_act):
    squashed = 1.0 / (1.0 + jnp.exp(-pre_act))
    return squashed * (1.0 + pre_act * (1.0 - squashed))


def halves(value):
    high = value.astype(BF16)
    low = (value - high.astype(F32)).astype(BF16)
    return jnp.concatenate([high, low], axis=0)


def fold(value):
    rows = value.shape[0] // 2
    return value[:rows] + value[rows:]


def inverse_factor(gram):
    rank = gram.shape[0]
    rows = lax.broadcasted_iota(jnp.int32, (rank, rank), 0)
    cols = lax.broadcasted_iota(jnp.int32, (rank, rank), 1)
    left = gram
    right = (rows == cols).astype(F32)
    row_id = lax.broadcasted_iota(jnp.int32, (rank, 1), 0)
    for i in range(rank - 1):
        scale = 1.0 / left[i : i + 1, i : i + 1]
        col = jnp.where(row_id > i, left[:, i : i + 1], 0.0)
        row_l = left[i : i + 1, :] * scale
        row_r = right[i : i + 1, :] * scale
        left = left - col * row_l
        right = right - col * row_r
    pivots = jnp.sum(jnp.where(rows == cols, left, 0.0), axis=1, keepdims=True)
    return right * (1.0 / jnp.sqrt(pivots))


def kernel(dims, tok_hbm, gh_hbm, rt_hbm, gt_hbm, w_hbm, err_hbm, q_hbm,
           gt_out, err_out, wg_out,
           tok_all, gh_raw, gh_sel, gh_all, rt_v, gt_v, gate_sel, gate_all, w_all, x_all, gp_all,
           err_v, merged, merged_b, back, ret, q_v, q2, facc, fbuf, rsbuf, agbuf, tbuf, bt_v,
           in_s, tok_s, tok_r, gh_s, gh_r, gate_s, gate_r, w_s, w_r,
           f_s, f_r, a_s, a_r, t_s, t_r, b_s, b_r):
    E, N, rp, chunk, gather_w, C, CB = dims
    z = lax.axis_index("expert")
    me = lax.axis_index("dp")
    tokens, width = tok_hbm.shape
    shard = width // N
    rank = q_hbm.shape[0]
    groups = width // 128
    part = tokens // C
    back_part = tokens // CB

    def other(axis, size, k):
        return lax.rem(lax.axis_index(axis) + k, size)

    def loop(size, fn, start=1):
        def step(k, c):
            fn(k)
            return c
        lax.fori_loop(start, size, step, 0)

    barrier = pltpu.get_barrier_semaphore()
    loop(E, lambda k: pl.semaphore_signal(
        barrier, inc=1, device_id={"expert": other("expert", E, k)}, device_id_type=MESH))
    loop(N, lambda k: pl.semaphore_signal(
        barrier, inc=1, device_id={"dp": other("dp", N, k)}, device_id_type=MESH))

    def w_rows(slot):
        return w_all.at[pl.ds(pl.multiple_of(slot * shard, 16), shard)] if gather_w else w_all

    loads = [
        pltpu.make_async_copy(tok_hbm, tok_all.at[z], in_s.at[0]),
        pltpu.make_async_copy(w_hbm, w_rows(me), in_s.at[1]),
        pltpu.make_async_copy(rt_hbm, rt_v, in_s.at[2]),
        pltpu.make_async_copy(gt_hbm, gt_v, in_s.at[3]),
        pltpu.make_async_copy(gh_hbm, gh_raw, in_s.at[4]),
        pltpu.make_async_copy(q_hbm, q_v, in_s.at[5]),
        pltpu.make_async_copy(err_hbm.at[0, 0], err_v, in_s.at[6]),
    ]
    for load in loads:
        load.start()

    def rdma(src, dst, s, r, axis, peer):
        return pltpu.make_async_remote_copy(
            src_ref=src, dst_ref=dst, send_sem=s, recv_sem=r,
            device_id={axis: peer}, device_id_type=MESH)

    def gate_copy(p, slot, k):
        return rdma(gate_sel.at[p], gate_all.at[slot], gate_s.at[k], gate_r.at[slot], "expert", p)

    def gh_copy(p, slot, k):
        return rdma(gh_sel.at[p], gh_all.at[slot], gh_s.at[k], gh_r.at[slot], "expert", p)

    def rows_of(c):
        return pl.ds(pl.multiple_of(c * part, 16), part)

    def tok_copy(j, c, nb, d):
        piece = tok_all.at[j, rows_of(c)]
        return rdma(piece, piece, tok_s.at[d, j], tok_r.at[j, c], "expert", nb)

    def w_copy(p, slot, k):
        return rdma(w_rows(slot), w_rows(slot), w_s.at[k], w_r.at[slot], "dp", p)

    def each(p_axis, size, copy, act):
        mine = lax.axis_index(p_axis)

        def fn(k):
            p = other(p_axis, size, k)
            if act == "start":
                copy(p, mine, k).start()
            elif act == "recv":
                copy(p, p, k).wait_recv()
            else:
                copy(p, mine, k).wait_send()
        loop(size, fn)

    partner = me + 1 - 2 * lax.rem(me, 2)
    half = N // 2

    def cross(k):
        return me + 2 * (lax.bitwise_xor(me // 2, k) - me // 2)

    for i in range(4):
        loads[i].wait()
    pl.semaphore_wait(barrier, E - 1 + N - 1)

    for d, dirn in enumerate((1, -1)):
        nb = z + dirn

        @pl.when((nb >= 0) & (nb < E))
        def _():
            loop(C, lambda c: tok_copy(z, c, nb, d).start(), 0)
    if gather_w:
        loop(half, lambda k: w_copy(cross(k), me, k).start())
        w_copy(partner, me, 0).start()

    routes = rt_v[...]
    gates = gt_v[...]

    def pick_gate(e):
        row = jnp.where(routes[0:1] == e, gates[0:1], jnp.where(routes[1:2] == e, gates[1:2], 0.0))
        gate_sel[e] = jnp.broadcast_to(row, (8, tokens))
    loop(E, pick_gate, 0)
    each("expert", E, gate_copy, "start")
    gate_all[z] = gate_sel[z]

    loads[4].wait()
    pairs = gh_raw[...].reshape(2 * tokens, gh_raw.shape[2])
    named = jnp.transpose(jnp.concatenate([routes.astype(F32)] * 4, axis=0))
    t_id = lax.broadcasted_iota(jnp.int32, (tokens, 2 * tokens), 0)
    p_id = lax.broadcasted_iota(jnp.int32, (tokens, 2 * tokens), 1)
    wanted = jnp.where(p_id == 2 * t_id, named[:, 0:1],
                       jnp.where(p_id == 2 * t_id + 1, named[:, 1:2], -1.0))

    def pick_rows(e):
        choose = jnp.where(wanted == e.astype(F32), 1.0, 0.0).astype(BF16)
        gh_sel[e] = jnp.dot(choose, pairs, preferred_element_type=F32).astype(BF16)

    def gh_send(p):
        gh_copy(p, z, lax.rem(p - z + E, E)).start()

    loop(E, pick_rows, 0)
    gh_all[z] = gh_sel[z]

    def mirrored(value):
        return jnp.where(z < E - 1 - z, value, E - 1 - value)

    def act(op):
        kind = op[0]
        if kind == "g":
            gh_send(mirrored(op[1]))
        elif kind == "w":
            tok_copy(mirrored(op[1]), op[2], z, 0).wait_recv()
        elif kind == "r":
            dirn = jnp.where(z < E - 1 - z, op[1], -op[1])
            tok_copy(mirrored(op[2]), op[3], z + dirn, jnp.where(dirn > 0, 0, 1)).start()
        elif gather_w:
            weights()

    def acts(pick):
        for low in range(E // 2):
            @pl.when((z == low) | (z == E - 1 - low))
            def _():
                pick(low)

    def look(table, k):
        code = table[0]
        for n in range(1, len(table)):
            code = jnp.where(k == n, table[n], code)
        return code

    if E == len(PLAN) * 2:
        acts(lambda low: [act(op) for op in PLAN[low][0]])
    else:
        loop(E, lambda k: gh_send(other("expert", E, k)))

    loads[5].wait()
    loads[6].wait()
    q2[...] = halves(q_v[...])

    def err_factor(c):
        cols = pl.ds(pl.multiple_of(c * chunk, chunk), chunk)
        facc[:, cols] = fold(lax.dot_general(
            q2[...], err_v[cols, :], NT, preferred_element_type=F32))
    loop(width // chunk, err_factor, 0)

    def back_rows(c):
        return pl.ds(pl.multiple_of(c * back_part, 16), back_part)

    def back_copy(dest, c):
        dirn = jnp.where(dest > z, 1, -1)
        nb = z + dirn
        slot = jnp.where((dest == nb) & (dest < z), E, dest)
        return rdma(back.at[dest, back_rows(c)], ret.at[slot, back_rows(c)],
                    b_s.at[dest], b_r.at[slot, c], "expert", nb)

    def back_wait(slot, c):
        rdma(back.at[0, back_rows(c)], ret.at[slot, back_rows(c)], b_s.at[0], b_r.at[slot, c],
             "expert", other("expert", E, 1)).wait_recv()

    def add_back(dest, slot, c):
        rows = back_rows(c)
        back[dest, rows, :] = (back[dest, rows, :].astype(F32)
                               + ret[slot, rows, :].astype(F32)).astype(BF16)

    unit = tokens // 2

    def unit_rows(h):
        return pl.ds(pl.multiple_of(h * unit, 16), unit)

    def gate_column(j, h):
        column = jnp.transpose(gate_all[j])[:, :1]
        return jnp.where(h == 0, column[:unit], column[unit:])

    def inward(j, h, fresh):
        @pl.when((j != z) & fresh)
        def _():
            gate_copy(j, j, 0).wait_recv()
            gh_copy(j, j, 0).wait_recv()
        rows = unit_rows(h)
        x = (tok_all[j, rows, :].astype(F32) * gate_column(j, h)).astype(BF16)
        x_all[j, rows, :] = x
        pre = jnp.dot(x, w_all[...], preferred_element_type=F32)
        gp = (gh_all[j, rows, :].astype(F32) * slopes(pre)).astype(BF16)
        gp_all[j, rows, :] = gp
        seen = fold(lax.dot_general(q2[...], gp, NT, preferred_element_type=F32))
        facc[...] += fold(jnp.dot(halves(seen), x, preferred_element_type=F32))

    def outward(j, h):
        rows = unit_rows(h)
        back[j, rows, :] = (lax.dot_general(gp_all[j, rows, :], w_all[...], NT,
                                            preferred_element_type=F32)
                            * gate_column(j, h)).astype(BF16)

        @pl.when(((j > z) & (z == 0)) | ((j < z) & (z == E - 1)))
        def _():
            loop(CB // 2, lambda c: back_copy(j, h * (CB // 2) + c).start(), 0)

    def forward(s):
        def piece(c):
            for d, dirn in enumerate((1, -1)):
                j = z - dirn * s
                nb = z + dirn

                @pl.when((j >= 0) & (j < E))
                def _():
                    tok_copy(j, c, z, d).wait_recv()

                    @pl.when((nb >= 0) & (nb < E))
                    def _():
                        tok_copy(j, c, nb, d).start()
        loop(C, piece, 0)

    def weights():
        def pass_on(k):
            w_copy(cross(k), cross(k), 0).wait_recv()
            w_copy(partner, cross(k), half + k).start()
        loop(half, pass_on)
        w_copy(partner, partner, 0).wait_recv()
        loop(half, lambda k: w_copy(partner, partner + cross(k) - me, 0).wait_recv())

    if E == len(PLAN) * 2:
        turns = len(PLAN[0]) - 1

        def unit_at(k):
            codes = [[4 * op[1] + 2 * op[2] + op[3] for op in (turn[-1] for turn in side[1:])]
                     for side in PLAN]
            code = jnp.where((z == 0) | (z == E - 1), look(codes[0], k), look(codes[1], k))
            return mirrored(code // 4), lax.rem(code // 2, 2), lax.rem(code, 2) == 1

        def turn(k):
            def moves(low):
                for n in range(turns):
                    ops = PLAN[low][n + 1][:-1]
                    if ops:
                        @pl.when(k == n)
                        def _():
                            for op in ops:
                                act(op)
            acts(moves)
            j, h, fresh = unit_at(k)
            inward(j, h, fresh)

            @pl.when(k < turns - 1)
            def _():
                outward(j, h)
        loop(turns, turn, 0)
    else:
        def step(s):
            forward(s)
            if gather_w:
                @pl.when(s == 1)
                def _():
                    weights()

            def block(i, carry):
                side = i // 2
                h = lax.rem(i, 2)
                j = jnp.where(side == 0, z, jnp.where(side == 1, z - s, z + s))

                @pl.when((j >= 0) & (j < E) & ((side > 0) | (s == 1)))
                def _():
                    inward(j, h, h == 0)
                    outward(j, h)
                return carry
            lax.fori_loop(0, 6, block, 0)
        loop(E, step)

    if fbuf.shape[0] > groups * rank:
        fbuf[groups * rank :, :] = jnp.zeros((fbuf.shape[0] - groups * rank, 128), BF16)
    for c in range(groups):
        fbuf[c * rank : (c + 1) * rank, :] = facc[:, c * 128 : (c + 1) * 128].astype(BF16)

    def f_copy(p, slot, k):
        return rdma(fbuf.at[pl.ds(pl.multiple_of(p * rp, 16), rp)], rsbuf.at[slot],
                    f_s.at[k], f_r.at[slot], "dp", p)

    def a_copy(p, slot, k):
        piece = agbuf.at[pl.ds(pl.multiple_of(slot * rp, 16), rp)]
        return rdma(piece, piece, a_s.at[k], a_r.at[slot], "dp", p)

    def t_copy(p, slot, k):
        return rdma(tbuf.at[slot], tbuf.at[slot], t_s.at[k], t_r.at[slot], "dp", p)

    own = pl.ds(pl.multiple_of(me * rp, 16), rp)
    each("dp", N, f_copy, "start")
    rsbuf[me] = fbuf[own, :]

    if E == len(PLAN) * 2:
        j, h, _ = unit_at(turns - 1)
        outward(j, h)

    right_first = z < E - 1 - z
    lag = 3

    def relay(m, c):
        def turn(i, carry):
            right = (i == 0) == right_first
            dest = jnp.where(right, m, E - 1 - m)
            hop = jnp.where(right, (dest > z) & (z > 0), (dest < z) & (z < E - 1))
            piece = c - lag * i

            @pl.when(hop & (piece >= 0) & (piece < CB))
            def _():
                back_wait(dest, piece)
                add_back(dest, dest, piece)
                back_copy(dest, piece).start()
            return carry
        lax.fori_loop(0, 2, turn, 0)

    def planned(start, stop):
        @pl.when((z > 0) & (z < E - 1))
        def _():
            def one(i, carry):
                code = look([CB * op[0] + op[1] for op in RELAYS], i)
                dest = mirrored(code // CB)
                piece = lax.rem(code, CB)
                back_wait(dest, piece)
                add_back(dest, dest, piece)
                back_copy(dest, piece).start()
                return carry
            lax.fori_loop(start, stop, one, 0)

    def relays(start, stop, first, last):
        def rank_of(m, carry):
            loop(last, lambda c: relay(m, c), first)
            return carry
        lax.fori_loop(start, stop, rank_of, 0)

    def merge(c):
        cols = pl.ds(pl.multiple_of(c * chunk, chunk), chunk)
        x = x_all[:, :, cols].reshape(E * tokens, chunk)
        gp = gp_all[...].reshape(E * tokens, gp_all.shape[2])
        m = lax.dot_general(x, gp, TN, preferred_element_type=F32)
        m = m + err_v[cols, :].astype(F32)
        merged[cols, :] = m
        merged_b[cols, :] = m.astype(BF16)
    if E == len(PLAN) * 2:
        planned(0, STOPS[0])
    else:
        relays(1, E - 1, 0, CB // 2)
    each("dp", N, f_copy, "recv")
    agbuf[own, :] = (jnp.sum(rsbuf[...].astype(F32), axis=0) * (1.0 / N)).astype(BF16)
    each("dp", N, a_copy, "start")
    loop(width // chunk, merge, 0)

    if E == len(PLAN) * 2:
        planned(STOPS[0], STOPS[1])
    else:
        relays(1, E - 1, CB // 2, CB + lag)
    each("dp", N, a_copy, "recv")
    factor = jnp.concatenate([agbuf[c * rank : (c + 1) * rank, :] for c in range(groups)], axis=1)
    tbuf[me] = jnp.dot(factor, merged_b[...], preferred_element_type=F32).astype(BF16)
    each("dp", N, t_copy, "start")

    if E == len(PLAN) * 2:
        planned(STOPS[1], STOPS[2])
    gram = lax.dot_general(factor, factor, NT, preferred_element_type=F32)
    inverse = inverse_factor(gram)
    basis = fold(jnp.dot(halves(inverse), factor, preferred_element_type=F32))
    bt_v[...] = jnp.transpose(basis).astype(BF16)

    if E == len(PLAN) * 2:
        planned(STOPS[2], len(RELAYS))
    else:
        relays(E - 1, E, 0, CB + lag)
    for d, dirn in enumerate((1, -1)):
        nb = z + dirn
        ahead = z if d == 0 else E - 1 - z

        @pl.when((nb >= 0) & (nb < E))
        def _():
            def drain(s):
                @pl.when(s <= ahead)
                def _():
                    j = z - dirn * s
                    rdma(tok_all.at[j], tok_all.at[j], tok_s.at[d, j], tok_r.at[j, 0],
                         "expert", nb).wait_send()
            loop(E, drain, 0)
    each("expert", E, gate_copy, "send")
    each("expert", E, gh_copy, "send")
    if gather_w:
        loop(half, lambda k: w_copy(cross(k), me, k).wait_send())
        w_copy(partner, me, 0).wait_send()
        loop(half, lambda k: w_copy(partner, cross(k), half + k).wait_send())
    each("dp", N, f_copy, "send")
    each("dp", N, a_copy, "send")
    each("dp", N, t_copy, "recv")
    mean = jnp.sum(tbuf[...].astype(F32), axis=0) * (1.0 / N)
    q_factor = jnp.dot(inverse, mean, precision=HI, preferred_element_type=F32).astype(BF16)

    for c in range(width // chunk):
        cols = pl.ds(c * chunk, chunk)
        low = jnp.dot(bt_v[cols, :], q_factor, preferred_element_type=F32)
        err_out[0, 0, cols, :] = (merged[cols, :] - low).astype(BF16)
    wg_out[0] = jnp.dot(bt_v[pl.ds(pl.multiple_of(me * shard, 8), shard), :], q_factor,
                        preferred_element_type=F32)

    @pl.when(z > 0)
    def _():
        def piece(c):
            back_wait(z, c)
            add_back(z, z, c)
        loop(CB, piece, 0)

    @pl.when(z < E - 1)
    def _():
        def piece(c):
            back_wait(E, c)
            add_back(z, E, c)
        loop(CB, piece, 0)
    gt_out[...] = back[z]

    def sent(k):
        dest = other("expert", E, k)
        rdma(back.at[dest], ret.at[dest], b_s.at[dest], b_r.at[dest, 0], "expert",
             other("expert", E, 1)).wait_send()
    loop(E, sent)
    each("dp", N, t_copy, "send")


def body(tokens, routes, gates, grad_hidden, w_in, error, q_seed):
    E = lax.axis_size("expert")
    N = lax.axis_size("dp")
    rows, width = tokens.shape
    hidden = grad_hidden.shape[2]
    rank = q_seed.shape[2]
    shard = width // N
    gather_w = shard % 16 == 0 and N & (N - 1) == 0
    weight = w_in[0] if gather_w else lax.all_gather(w_in[0], "dp", axis=0, tiled=True)
    chunk = 256 if width % 256 == 0 else 128
    C, CB = (4, 8) if E <= 8 else (2, 2)
    room = (4 * E + 3) * rows * width * 2 + 3 * E * rows * hidden * 2 + 13 * width * hidden + (12 << 20)
    total_rows = width // 128 * rank
    rp = -(-total_rows // N)
    rp = -(-rp // 16) * 16
    dma = pltpu.SemaphoreType.DMA
    vmem = pl.BlockSpec(memory_space=pltpu.VMEM)
    hbm = pl.BlockSpec(memory_space=pltpu.HBM)
    return pl.pallas_call(
        functools.partial(kernel, (E, N, rp, chunk, gather_w, C, CB)),
        out_shape=(
            jax.ShapeDtypeStruct((rows, width), BF16),
            jax.ShapeDtypeStruct((1, 1, width, hidden), BF16),
            jax.ShapeDtypeStruct((1, shard, hidden), F32),
        ),
        in_specs=[hbm] * 7,
        out_specs=(vmem, vmem, vmem),
        scratch_shapes=[
            pltpu.VMEM((E, rows, width), BF16),
            pltpu.VMEM((rows, 2, hidden), BF16),
            pltpu.VMEM((E, rows, hidden), BF16),
            pltpu.VMEM((E, rows, hidden), BF16),
            pltpu.VMEM((2, rows), jnp.int32),
            pltpu.VMEM((2, rows), F32),
            pltpu.VMEM((E, 8, rows), F32),
            pltpu.VMEM((E, 8, rows), F32),
            pltpu.VMEM((width, hidden), BF16),
            pltpu.VMEM((E, rows, width), BF16),
            pltpu.VMEM((E, rows, hidden), BF16),
            pltpu.VMEM((width, hidden), BF16),
            pltpu.VMEM((width, hidden), F32),
            pltpu.VMEM((width, hidden), BF16),
            pltpu.VMEM((E, rows, width), BF16),
            pltpu.VMEM((E + 1, rows, width), BF16),
            pltpu.VMEM((rank, hidden), F32),
            pltpu.VMEM((2 * rank, hidden), BF16),
            pltpu.VMEM((rank, width), F32),
            pltpu.VMEM((rp * N, 128), BF16),
            pltpu.VMEM((N, rp, 128), BF16),
            pltpu.VMEM((rp * N, 128), BF16),
            pltpu.VMEM((N, rank, hidden), BF16),
            pltpu.VMEM((width, rank), BF16),
            dma((7,)), dma((2, E)), dma((E, C)), dma((E,)), dma((E,)), dma((E,)), dma((E,)),
            dma((N,)), dma((N,)), dma((N,)), dma((N,)), dma((N,)), dma((N,)), dma((N,)), dma((N,)),
            dma((E,)), dma((E + 1, CB)),
        ],
        compiler_params=pltpu.CompilerParams(
            collective_id=0, has_side_effects=True, vmem_limit_bytes=min(room, 67043328 - (1 << 20))),
    )(*(pltpu.with_memory_space_constraint(a, pltpu.HBM) for a in (
        tokens, grad_hidden, routes.T, gates.T, weight, error, q_seed[0].T)))


def solution(mesh):
    placed = (
        P(("dp", "expert"), None),
        P(("dp", "expert"), None),
        P(("dp", "expert"), None),
        P(("dp", "expert"), None, None),
        P("expert", "dp", None),
        P("dp", "expert", None, None),
        P("expert", None, None),
    )
    return jax.shard_map(
        body,
        mesh=mesh,
        in_specs=placed,
        out_specs=(
            P(("dp", "expert"), None),
            P("dp", "expert", None, None),
            P("expert", "dp", None),
        ),
        check_vma=False,
    )
```

```python
import functools

import jax
import jax.numpy as jnp
from jax import lax
from jax.experimental import pallas as pl
from jax.experimental.pallas import tpu as pltpu
from jax.sharding import PartitionSpec as P

HI = lax.Precision.HIGHEST
MESH = pl.DeviceIdType.MESH
F32 = jnp.float32
BF16 = jnp.bfloat16
NT = (((1,), (1,)), ((), ()))
TN = (((0,), (0,)), ((), ()))


PLAN = (
    (
        (("g", 1), ("g", 2), ("g", 3),),
        (("w", 1, 0), ("w", 1, 1), ("w", 1, 2), ("w", 1, 3), ("W",), ("u", 1, 0, 1),),
        (("u", 1, 1, 0),),
        (("u", 0, 0, 1),),
        (("u", 0, 1, 0),),
        (("w", 2, 0), ("w", 2, 1), ("u", 2, 0, 1),),
        (("w", 3, 0), ("w", 3, 1), ("u", 3, 0, 1),),
        (("w", 3, 2), ("w", 3, 3), ("u", 3, 1, 0),),
        (("w", 2, 2), ("w", 2, 3), ("u", 2, 1, 0),),
    ),
    (
        (("g", 0), ("g", 2), ("g", 3),),
        (("w", 0, 0), ("r", 1, 0, 0), ("w", 2, 0), ("r", -1, 2, 0), ("w", 0, 1), ("r", 1, 0, 1), ("w", 2, 1), ("r", -1, 2, 1), ("w", 0, 2), ("r", 1, 0, 2), ("w", 2, 2), ("r", -1, 2, 2), ("w", 0, 3), ("r", 1, 0, 3), ("w", 2, 3), ("W",), ("u", 1, 0, 1),),
        (("u", 1, 1, 0),),
        (("u", 0, 0, 1),),
        (("u", 0, 1, 0),),
        (("u", 2, 0, 1),),
        (("u", 2, 1, 0),),
        (("w", 3, 0), ("r", -1, 3, 0), ("w", 3, 1), ("r", -1, 3, 1), ("u", 3, 0, 1),),
        (("w", 3, 2), ("r", -1, 3, 2), ("w", 3, 3), ("r", -1, 3, 3), ("r", -1, 2, 3), ("u", 3, 1, 0),),
    ),
)
RELAYS = (
    (2, 0), (2, 1), (2, 2), (2, 3), (3, 0), (3, 1), (3, 2), (3, 3),
    (0, 0), (3, 4), (0, 1), (3, 5), (0, 2), (3, 6), (0, 3), (3, 7),
    (0, 4), (2, 4), (0, 5), (2, 5), (0, 6), (2, 6), (0, 7), (2, 7),
)
STOPS = (4, 7, 9, 11, 13, 15)


def slopes(pre_act):
    squashed = 1.0 / (1.0 + jnp.exp(-pre_act))
    return squashed * (1.0 + pre_act * (1.0 - squashed))


def halves(value):
    high = value.astype(BF16)
    low = (value - high.astype(F32)).astype(BF16)
    return jnp.concatenate([high, low], axis=0)


def fold(value):
    rows = value.shape[0] // 2
    return value[:rows] + value[rows:]


def inverse_factor(gram, between):
    rank = gram.shape[0]
    rows = lax.broadcasted_iota(jnp.int32, (rank, rank), 0)
    cols = lax.broadcasted_iota(jnp.int32, (rank, rank), 1)
    left = gram
    right = (rows == cols).astype(F32)
    row_id = lax.broadcasted_iota(jnp.int32, (rank, 1), 0)
    for i in range(rank - 1):
        scale = 1.0 / left[i : i + 1, i : i + 1]
        col = jnp.where(row_id > i, left[:, i : i + 1], 0.0)
        row_l = left[i : i + 1, :] * scale
        row_r = right[i : i + 1, :] * scale
        left = left - col * row_l
        right = right - col * row_r
        if i % 8 == 7:
            between(i // 8)
    pivots = jnp.sum(jnp.where(rows == cols, left, 0.0), axis=1, keepdims=True)
    return right * (1.0 / jnp.sqrt(pivots))


def kernel(dims, tok_hbm, gh_hbm, rt_hbm, gt_hbm, w_hbm, err_hbm, q_hbm,
           gt_out, merged, bt_v, q_out,
           tok_all, gh_raw, gh_sel, gh_all, rt_v, gt_v, gate_sel, gate_all, w_all, x_all, gp_all,
           err_v, merged_b, back, ret, q_v, q2, facc, fbuf, rsbuf, agbuf, tbuf,
           in_s, tok_s, tok_r, gh_s, gh_r, gate_s, gate_r, w_s, w_r,
           f_s, f_r, a_s, a_r, t_s, t_r, b_s, b_r):
    E, N, rp, chunk, gather_w, C, CB = dims
    z = lax.axis_index("expert")
    me = lax.axis_index("dp")
    tokens, width = tok_hbm.shape
    shard = width // N
    rank = q_hbm.shape[0]
    groups = width // 128
    part = tokens // C
    back_part = tokens // CB

    def other(axis, size, k):
        return lax.rem(lax.axis_index(axis) + k, size)

    def loop(size, fn, start=1):
        def step(k, c):
            fn(k)
            return c
        lax.fori_loop(start, size, step, 0)

    barrier = pltpu.get_barrier_semaphore()
    for axis, size in (("expert", E), ("dp", N)):
        for k in range(1, size):
            pl.semaphore_signal(barrier, inc=1, device_id={axis: other(axis, size, k)},
                                device_id_type=MESH)

    def w_rows(slot):
        return w_all.at[pl.ds(pl.multiple_of(slot * shard, 16), shard)] if gather_w else w_all

    loads = [
        pltpu.make_async_copy(tok_hbm, tok_all.at[z], in_s.at[0]),
        pltpu.make_async_copy(w_hbm, w_rows(me), in_s.at[1]),
        pltpu.make_async_copy(rt_hbm, rt_v, in_s.at[2]),
        pltpu.make_async_copy(gt_hbm, gt_v, in_s.at[3]),
        pltpu.make_async_copy(gh_hbm, gh_raw, in_s.at[4]),
        pltpu.make_async_copy(q_hbm, q_v, in_s.at[5]),
        pltpu.make_async_copy(err_hbm.at[0, 0], err_v, in_s.at[6]),
    ]
    for load in loads:
        load.start()

    def rdma(src, dst, s, r, axis, peer):
        return pltpu.make_async_remote_copy(
            src_ref=src, dst_ref=dst, send_sem=s, recv_sem=r,
            device_id={axis: peer}, device_id_type=MESH)

    def gate_copy(p, slot, k):
        return rdma(gate_sel.at[p], gate_all.at[slot], gate_s, gate_r.at[slot], "expert", p)

    def gh_copy(p, slot, k):
        return rdma(gh_sel.at[p], gh_all.at[slot], gh_s, gh_r.at[slot], "expert", p)

    def rows_of(c):
        return pl.ds(pl.multiple_of(c * part, 16), part)

    def tok_copy(j, c, nb, d):
        piece = tok_all.at[j, rows_of(c)]
        return rdma(piece, piece, tok_s.at[d, j], tok_r.at[j, c], "expert", nb)

    def w_copy(p, slot, k):
        return rdma(w_rows(slot), w_rows(slot), w_s, w_r.at[slot], "dp", p)

    def each(p_axis, size, copy, act):
        mine = lax.axis_index(p_axis)

        def fn(k):
            p = other(p_axis, size, k)
            if act == "start":
                copy(p, mine, k).start()
            elif act == "recv":
                copy(p, p, k).wait_recv()
            else:
                copy(p, mine, k).wait_send()
        loop(size, fn)

    partner = me + 1 - 2 * lax.rem(me, 2)
    half = N // 2

    def cross(k):
        return me + 2 * (lax.bitwise_xor(me // 2, k) - me // 2)

    for i in range(4):
        loads[i].wait()
    pl.semaphore_wait(barrier, E - 1 + N - 1)

    for d, dirn in enumerate((1, -1)):
        nb = z + dirn

        @pl.when((nb >= 0) & (nb < E))
        def _():
            loop(C, lambda c: tok_copy(z, c, nb, d).start(), 0)
    if gather_w:
        loop(half, lambda k: w_copy(cross(k), me, k).start())
        w_copy(partner, me, 0).start()

    routes = rt_v[...]
    gates = gt_v[...]

    def pick_gate(e):
        row = jnp.where(routes[0:1] == e, gates[0:1], jnp.where(routes[1:2] == e, gates[1:2], 0.0))
        gate_sel[e] = jnp.broadcast_to(row, (8, tokens))
    loop(E, pick_gate, 0)
    each("expert", E, gate_copy, "start")
    gate_all[z] = gate_sel[z]

    loads[4].wait()
    pairs = gh_raw[...].reshape(2 * tokens, gh_raw.shape[2])
    named = jnp.transpose(jnp.concatenate([routes.astype(F32)] * 4, axis=0))
    t_id = lax.broadcasted_iota(jnp.int32, (tokens, 2 * tokens), 0)
    p_id = lax.broadcasted_iota(jnp.int32, (tokens, 2 * tokens), 1)
    wanted = jnp.where(p_id == 2 * t_id, named[:, 0:1],
                       jnp.where(p_id == 2 * t_id + 1, named[:, 1:2], -1.0))

    def pick_rows(e):
        choose = jnp.where(wanted == e.astype(F32), 1.0, 0.0).astype(BF16)
        gh_sel[e] = jnp.dot(choose, pairs, preferred_element_type=F32).astype(BF16)

    def gh_send(p):
        gh_copy(p, z, lax.rem(p - z + E, E)).start()

    loop(E, pick_rows, 0)
    gh_all[z] = gh_sel[z]

    def mirrored(value):
        return jnp.where(z < E - 1 - z, value, E - 1 - value)

    def act(op):
        kind = op[0]
        if kind == "g":
            gh_send(mirrored(op[1]))
        elif kind == "w":
            tok_copy(mirrored(op[1]), op[2], z, 0).wait_recv()
        elif kind == "r":
            dirn = jnp.where(z < E - 1 - z, op[1], -op[1])
            tok_copy(mirrored(op[2]), op[3], z + dirn, jnp.where(dirn > 0, 0, 1)).start()
        elif kind == "x":
            pass_on(mirrored(op[1]), op[2])
        elif gather_w:
            weights()

    def acts(pick):
        for low in range(E // 2):
            @pl.when((z == low) | (z == E - 1 - low))
            def _():
                pick(low)

    def look(table, k):
        code = table[0]
        for n in range(1, len(table)):
            code = jnp.where(k == n, table[n], code)
        return code

    if E == len(PLAN) * 2:
        acts(lambda low: [act(op) for op in PLAN[low][0]])
    else:
        loop(E, lambda k: gh_send(other("expert", E, k)))

    loads[5].wait()
    loads[6].wait()
    q2[...] = halves(q_v[...])

    def err_factor(c):
        cols = pl.ds(pl.multiple_of(c * chunk, chunk), chunk)
        facc[:, cols] = fold(lax.dot_general(
            q2[...], err_v[cols, :], NT, preferred_element_type=F32))
    loop(width // chunk, err_factor, 0)

    def back_rows(c):
        return pl.ds(pl.multiple_of(c * back_part, 16), back_part)

    def back_copy(dest, c):
        dirn = jnp.where(dest > z, 1, -1)
        nb = z + dirn
        slot = jnp.where((dest == nb) & (dest < z), E, dest)
        return rdma(back.at[dest, back_rows(c)], ret.at[slot, back_rows(c)],
                    b_s.at[dest], b_r.at[slot, c], "expert", nb)

    def back_wait(slot, c):
        rdma(back.at[0, back_rows(c)], ret.at[slot, back_rows(c)], b_s.at[0], b_r.at[slot, c],
             "expert", other("expert", E, 1)).wait_recv()

    def add_back(dest, slot, c):
        rows = back_rows(c)
        back[dest, rows, :] = (back[dest, rows, :].astype(F32)
                               + ret[slot, rows, :].astype(F32)).astype(BF16)

    def pass_on(dest, piece):
        back_wait(dest, piece)
        add_back(dest, dest, piece)
        back_copy(dest, piece).start()

    unit = tokens // 2

    def unit_rows(h):
        return pl.ds(pl.multiple_of(h * unit, 16), unit)

    def gate_column(j, h):
        column = jnp.transpose(gate_all[j])[:, :1]
        return jnp.where(h == 0, column[:unit], column[unit:])

    def inward(j, h, fresh):
        @pl.when((j != z) & fresh)
        def _():
            gate_copy(j, j, 0).wait_recv()
            gh_copy(j, j, 0).wait_recv()
        rows = unit_rows(h)
        x = (tok_all[j, rows, :].astype(F32) * gate_column(j, h)).astype(BF16)
        x_all[j, rows, :] = x
        pre = jnp.dot(x, w_all[...], preferred_element_type=F32)
        gp = (gh_all[j, rows, :].astype(F32) * slopes(pre)).astype(BF16)
        gp_all[j, rows, :] = gp
        seen = fold(lax.dot_general(q2[...], gp, NT, preferred_element_type=F32))
        facc[...] += fold(jnp.dot(halves(seen), x, preferred_element_type=F32))

    def outward(j, h):
        rows = unit_rows(h)
        back[j, rows, :] = (lax.dot_general(gp_all[j, rows, :], w_all[...], NT,
                                            preferred_element_type=F32)
                            * gate_column(j, h)).astype(BF16)

        @pl.when(((j > z) & (z == 0)) | ((j < z) & (z == E - 1)))
        def _():
            loop(CB // 2, lambda c: back_copy(j, h * (CB // 2) + c).start(), 0)

    def forward(s):
        def piece(c):
            for d, dirn in enumerate((1, -1)):
                j = z - dirn * s
                nb = z + dirn

                @pl.when((j >= 0) & (j < E))
                def _():
                    tok_copy(j, c, z, d).wait_recv()

                    @pl.when((nb >= 0) & (nb < E))
                    def _():
                        tok_copy(j, c, nb, d).start()
        loop(C, piece, 0)

    def weights():
        def pass_on(k):
            w_copy(cross(k), cross(k), 0).wait_recv()
            w_copy(partner, cross(k), half + k).start()
        loop(half, pass_on)
        w_copy(partner, partner, 0).wait_recv()
        loop(half, lambda k: w_copy(partner, partner + cross(k) - me, 0).wait_recv())

    if E == len(PLAN) * 2:
        turns = len(PLAN[0]) - 1

        def unit_at(k):
            codes = [[4 * op[1] + 2 * op[2] + op[3] for op in (turn[-1] for turn in side[1:])]
                     for side in PLAN]
            code = jnp.where((z == 0) | (z == E - 1), look(codes[0], k), look(codes[1], k))
            return mirrored(code // 4), lax.rem(code // 2, 2), lax.rem(code, 2) == 1

        def turn(k):
            def moves(low):
                for n in range(turns):
                    ops = PLAN[low][n + 1][:-1]
                    if ops:
                        @pl.when(k == n)
                        def _():
                            for op in ops:
                                act(op)
            acts(moves)
            j, h, fresh = unit_at(k)
            inward(j, h, fresh)

            @pl.when(k < turns - 1)
            def _():
                outward(j, h)
        loop(turns, turn, 0)
    else:
        def step(s):
            forward(s)
            if gather_w:
                @pl.when(s == 1)
                def _():
                    weights()

            def block(i, carry):
                side = i // 2
                h = lax.rem(i, 2)
                j = jnp.where(side == 0, z, jnp.where(side == 1, z - s, z + s))

                @pl.when((j >= 0) & (j < E) & ((side > 0) | (s == 1)))
                def _():
                    inward(j, h, h == 0)
                    outward(j, h)
                return carry
            lax.fori_loop(0, 6, block, 0)
        loop(E, step)

    if fbuf.shape[0] > groups * rank:
        fbuf[groups * rank :, :] = jnp.zeros((fbuf.shape[0] - groups * rank, 128), BF16)
    for c in range(groups):
        fbuf[c * rank : (c + 1) * rank, :] = facc[:, c * 128 : (c + 1) * 128].astype(BF16)

    def f_copy(p, slot, k):
        return rdma(fbuf.at[pl.ds(pl.multiple_of(p * rp, 16), rp)], rsbuf.at[slot],
                    f_s, f_r, "dp", p)

    def a_copy(p, slot, k):
        piece = agbuf.at[pl.ds(pl.multiple_of(slot * rp, 16), rp)]
        return rdma(piece, piece, a_s, a_r, "dp", p)

    def t_copy(p, slot, k):
        return rdma(tbuf.at[slot], tbuf.at[slot], t_s, t_r, "dp", p)

    def all_f():
        return rdma(rsbuf.at[pl.ds(0, N - 1)], rsbuf.at[pl.ds(0, N - 1)], f_s, f_r, "dp", partner)

    def all_a():
        rest = agbuf.at[pl.ds(0, rp * (N - 1))]
        return rdma(rest, rest, a_s, a_r, "dp", partner)

    def all_t():
        return rdma(tbuf.at[pl.ds(0, N - 1)], tbuf.at[pl.ds(0, N - 1)], t_s, t_r, "dp", partner)

    own = pl.ds(pl.multiple_of(me * rp, 16), rp)
    each("dp", N, f_copy, "start")
    rsbuf[me] = fbuf[own, :]

    if E == len(PLAN) * 2:
        j, h, _ = unit_at(turns - 1)
        outward(j, h)

    right_first = z < E - 1 - z
    lag = 3

    def relay(m, c):
        def turn(i, carry):
            right = (i == 0) == right_first
            dest = jnp.where(right, m, E - 1 - m)
            hop = jnp.where(right, (dest > z) & (z > 0), (dest < z) & (z < E - 1))
            piece = c - lag * i

            @pl.when(hop & (piece >= 0) & (piece < CB))
            def _():
                back_wait(dest, piece)
                add_back(dest, dest, piece)
                back_copy(dest, piece).start()
            return carry
        lax.fori_loop(0, 2, turn, 0)

    def planned(start, stop):
        @pl.when((z > 0) & (z < E - 1))
        def _():
            def one(i, carry):
                code = look([CB * op[0] + op[1] for op in RELAYS], i)
                pass_on(mirrored(code // CB), lax.rem(code, CB))
                return carry
            lax.fori_loop(start, stop, one, 0)

    def relays(start, stop, first, last):
        def rank_of(m, carry):
            loop(last, lambda c: relay(m, c), first)
            return carry
        lax.fori_loop(start, stop, rank_of, 0)

    def merge(c):
        cols = pl.ds(pl.multiple_of(c * chunk, chunk), chunk)
        x = x_all[:, :, cols].reshape(E * tokens, chunk)
        gp = gp_all[...].reshape(E * tokens, gp_all.shape[2])
        m = lax.dot_general(x, gp, TN, preferred_element_type=F32)
        m = m + err_v[cols, :].astype(F32)
        merged[cols, :] = m
        merged_b[cols, :] = m.astype(BF16)
    if E == len(PLAN) * 2:
        planned(0, STOPS[0])
    else:
        relays(1, E - 1, 0, CB // 2)
    all_f().wait_recv()
    agbuf[own, :] = (jnp.sum(rsbuf[...].astype(F32), axis=0) * (1.0 / N)).astype(BF16)
    each("dp", N, a_copy, "start")
    loop(width // chunk, merge, 0)

    if E == len(PLAN) * 2:
        planned(STOPS[0], STOPS[1])
    else:
        relays(1, E - 1, CB // 2, CB + lag)
    all_a().wait_recv()
    factor = jnp.concatenate([agbuf[c * rank : (c + 1) * rank, :] for c in range(groups)], axis=1)
    tbuf[me] = jnp.dot(factor, merged_b[...], preferred_element_type=F32).astype(BF16)
    each("dp", N, t_copy, "start")

    if E == len(PLAN) * 2:
        planned(STOPS[1], STOPS[2])
    gram = lax.dot_general(factor, factor, NT, preferred_element_type=F32)
    def between(n):
        if E == len(PLAN) * 2 and n + 3 < len(STOPS):
            planned(STOPS[n + 2], STOPS[n + 3])
    inverse = inverse_factor(gram, between)
    basis = fold(jnp.dot(halves(inverse), factor, preferred_element_type=F32))
    bt_v[...] = jnp.transpose(basis).astype(BF16)

    if E == len(PLAN) * 2:
        planned(STOPS[-1], len(RELAYS))
    else:
        relays(E - 1, E, 0, CB + lag)
    for d, dirn in enumerate((1, -1)):
        nb = z + dirn
        ahead = z if d == 0 else E - 1 - z

        @pl.when((nb >= 0) & (nb < E))
        def _():
            def drain(s):
                @pl.when(s <= ahead)
                def _():
                    j = z - dirn * s
                    rdma(tok_all.at[j], tok_all.at[j], tok_s.at[d, j], tok_r.at[j, 0],
                         "expert", nb).wait_send()
            loop(E, drain, 0)
    rdma(gate_sel.at[pl.ds(0, E - 1)], gate_all.at[pl.ds(0, E - 1)], gate_s, gate_r.at[0],
         "expert", other("expert", E, 1)).wait_send()
    rdma(gh_sel.at[pl.ds(0, E - 1)], gh_all.at[pl.ds(0, E - 1)], gh_s, gh_r.at[0],
         "expert", other("expert", E, 1)).wait_send()
    if gather_w:
        rest = w_all.at[pl.ds(0, shard * (N - 1))]
        rdma(rest, rest, w_s, w_r.at[0], "dp", partner).wait_send()
    all_f().wait_send()
    all_a().wait_send()
    all_t().wait_recv()
    mean = jnp.sum(tbuf[...].astype(F32), axis=0) * (1.0 / N)
    q_out[...] = jnp.dot(inverse, mean, precision=HI, preferred_element_type=F32).astype(BF16)

    @pl.when(z > 0)
    def _():
        def piece(c):
            back_wait(z, c)
            add_back(z, z, c)
        loop(CB, piece, 0)

    @pl.when(z < E - 1)
    def _():
        def piece(c):
            back_wait(E, c)
            add_back(z, E, c)
        loop(CB, piece, 0)
    gt_out[...] = back[z]

    def sent(k):
        dest = other("expert", E, k)
        rdma(back.at[dest], ret.at[dest], b_s.at[dest], b_r.at[dest, 0], "expert",
             other("expert", E, 1)).wait_send()
    loop(E, sent)
    all_t().wait_send()


def finish(chunk, gt_v, merged, bt_v, q_v, gt_hbm, err_hbm, wg_hbm, err_v, wg_v, sem):
    width = merged.shape[0]
    shard = wg_v.shape[0]
    me = lax.axis_index("dp")
    count = width // chunk
    moves = [pltpu.make_async_copy(gt_v, gt_hbm, sem.at[0])]
    moves[0].start()
    wg_v[...] = jnp.dot(bt_v[pl.ds(pl.multiple_of(me * shard, 8), shard), :], q_v[...],
                        preferred_element_type=F32)
    moves.append(pltpu.make_async_copy(wg_v, wg_hbm.at[0], sem.at[1]))
    moves[1].start()
    for c in range(count):
        rows = pl.ds(c * chunk, chunk)
        low = jnp.dot(bt_v[rows, :], q_v[...], preferred_element_type=F32)
        err_v[rows, :] = (merged[rows, :] - low).astype(BF16)
        moves.append(pltpu.make_async_copy(err_v.at[rows], err_hbm.at[0, 0, rows], sem.at[2 + c]))
        moves[-1].start()
    for move in moves:
        move.wait()


def body(tokens, routes, gates, grad_hidden, w_in, error, q_seed):
    E = lax.axis_size("expert")
    N = lax.axis_size("dp")
    rows, width = tokens.shape
    hidden = grad_hidden.shape[2]
    rank = q_seed.shape[2]
    shard = width // N
    gather_w = shard % 16 == 0 and N & (N - 1) == 0
    weight = w_in[0] if gather_w else lax.all_gather(w_in[0], "dp", axis=0, tiled=True)
    chunk = 256 if width % 256 == 0 else 128
    C, CB = (4, 8) if E <= 8 else (2, 2)
    room = (4 * E + 3) * rows * width * 2 + 3 * E * rows * hidden * 2 + 13 * width * hidden + (12 << 20)
    total_rows = width // 128 * rank
    rp = -(-total_rows // N)
    rp = -(-rp // 16) * 16
    dma = pltpu.SemaphoreType.DMA
    vmem = pl.BlockSpec(memory_space=pltpu.VMEM)
    hbm = pl.BlockSpec(memory_space=pltpu.HBM)
    parts = pl.pallas_call(
        functools.partial(kernel, (E, N, rp, chunk, gather_w, C, CB)),
        out_shape=(
            jax.ShapeDtypeStruct((rows, width), BF16),
            jax.ShapeDtypeStruct((width, hidden), F32),
            jax.ShapeDtypeStruct((width, rank), BF16),
            jax.ShapeDtypeStruct((rank, hidden), BF16),
        ),
        in_specs=[hbm] * 7,
        out_specs=(vmem,) * 4,
        scratch_shapes=[
            pltpu.VMEM((E, rows, width), BF16),
            pltpu.VMEM((rows, 2, hidden), BF16),
            pltpu.VMEM((E, rows, hidden), BF16),
            pltpu.VMEM((E, rows, hidden), BF16),
            pltpu.VMEM((2, rows), jnp.int32),
            pltpu.VMEM((2, rows), F32),
            pltpu.VMEM((E, 8, rows), F32),
            pltpu.VMEM((E, 8, rows), F32),
            pltpu.VMEM((width, hidden), BF16),
            pltpu.VMEM((E, rows, width), BF16),
            pltpu.VMEM((E, rows, hidden), BF16),
            pltpu.VMEM((width, hidden), BF16),
            pltpu.VMEM((width, hidden), BF16),
            pltpu.VMEM((E, rows, width), BF16),
            pltpu.VMEM((E + 1, rows, width), BF16),
            pltpu.VMEM((rank, hidden), F32),
            pltpu.VMEM((2 * rank, hidden), BF16),
            pltpu.VMEM((rank, width), F32),
            pltpu.VMEM((rp * N, 128), BF16),
            pltpu.VMEM((N, rp, 128), BF16),
            pltpu.VMEM((rp * N, 128), BF16),
            pltpu.VMEM((N, rank, hidden), BF16),
            dma((7,)), dma((2, E)), dma((E, C)), dma(()), dma((E,)), dma(()), dma((E,)),
            dma(()), dma((N,)), dma(()), dma(()), dma(()), dma(()), dma(()), dma(()),
            dma((E,)), dma((E + 1, CB)),
        ],
        compiler_params=pltpu.CompilerParams(
            collective_id=0, has_side_effects=True, vmem_limit_bytes=min(room, 67043328 - (1 << 20))),
    )(*(pltpu.with_memory_space_constraint(a, pltpu.HBM) for a in (
        tokens, grad_hidden, routes.T, gates.T, weight, error, q_seed[0].T)))
    return pl.pallas_call(
        functools.partial(finish, chunk),
        out_shape=(
            jax.ShapeDtypeStruct((rows, width), BF16),
            jax.ShapeDtypeStruct((1, 1, width, hidden), BF16),
            jax.ShapeDtypeStruct((1, shard, hidden), F32),
        ),
        in_specs=[vmem] * 4,
        out_specs=(hbm, hbm, hbm),
        scratch_shapes=[
            pltpu.VMEM((width, hidden), BF16),
            pltpu.VMEM((shard, hidden), F32),
            dma((2 + width // chunk,)),
        ],
        compiler_params=pltpu.CompilerParams(vmem_limit_bytes=16 << 20),
    )(*parts)


def solution(mesh):
    placed = (
        P(("dp", "expert"), None),
        P(("dp", "expert"), None),
        P(("dp", "expert"), None),
        P(("dp", "expert"), None, None),
        P("expert", "dp", None),
        P("dp", "expert", None, None),
        P("expert", None, None),
    )
    return jax.shard_map(
        body,
        mesh=mesh,
        in_specs=placed,
        out_specs=(
            P(("dp", "expert"), None),
            P("dp", "expert", None, None),
            P("expert", "dp", None),
        ),
        check_vma=False,
    )
```

```python
import functools

import jax
import jax.numpy as jnp
from jax import lax
from jax.experimental import pallas as pl
from jax.experimental.pallas import tpu as pltpu
from jax.sharding import PartitionSpec as P

HI = lax.Precision.HIGHEST
MESH = pl.DeviceIdType.MESH
F32 = jnp.float32
BF16 = jnp.bfloat16
NT = (((1,), (1,)), ((), ()))
TN = (((0,), (0,)), ((), ()))


PLAN = (
    (
        (("g", 1), ("g", 2), ("g", 3),),
        (("w", 1, 0), ("w", 1, 1), ("w", 1, 2), ("w", 1, 3), ("W",), ("u", 1, 0, 1),),
        (("u", 1, 1, 0),),
        (("u", 0, 0, 1),),
        (("u", 0, 1, 0),),
        (("w", 2, 0), ("w", 2, 1), ("u", 2, 0, 1),),
        (("w", 3, 0), ("w", 3, 1), ("u", 3, 0, 1),),
        (("w", 3, 2), ("w", 3, 3), ("u", 3, 1, 0),),
        (("w", 2, 2), ("w", 2, 3), ("u", 2, 1, 0),),
    ),
    (
        (("g", 0), ("g", 2), ("g", 3),),
        (("w", 0, 0), ("r", 1, 0, 0), ("w", 2, 0), ("r", -1, 2, 0), ("w", 0, 1), ("r", 1, 0, 1), ("w", 2, 1), ("r", -1, 2, 1), ("w", 0, 2), ("r", 1, 0, 2), ("w", 2, 2), ("r", -1, 2, 2), ("w", 0, 3), ("r", 1, 0, 3), ("w", 2, 3), ("W",), ("u", 1, 0, 1),),
        (("u", 1, 1, 0),),
        (("u", 0, 0, 1),),
        (("u", 0, 1, 0),),
        (("u", 2, 0, 1),),
        (("u", 2, 1, 0),),
        (("w", 3, 0), ("r", -1, 3, 0), ("w", 3, 1), ("r", -1, 3, 1), ("u", 3, 0, 1),),
        (("w", 3, 2), ("r", -1, 3, 2), ("w", 3, 3), ("r", -1, 3, 3), ("r", -1, 2, 3), ("u", 3, 1, 0),),
    ),
)
RELAYS = (
    (2, 0), (2, 1), (2, 2), (2, 3), (3, 0), (3, 1), (3, 2), (3, 3),
    (0, 0), (3, 4), (0, 1), (3, 5), (0, 2), (3, 6), (0, 3), (3, 7),
    (0, 4), (2, 4), (0, 5), (2, 5), (0, 6), (2, 6), (0, 7), (2, 7),
)
STOPS = (4, 7, 8, 10, 12, 14)


def slopes(pre_act):
    squashed = 1.0 / (1.0 + jnp.exp(-pre_act))
    return squashed * (1.0 + pre_act * (1.0 - squashed))


def halves(value):
    high = value.astype(BF16)
    low = (value - high.astype(F32)).astype(BF16)
    return jnp.concatenate([high, low], axis=0)


def fold(value):
    rows = value.shape[0] // 2
    return value[:rows] + value[rows:]


def inverse_factor(gram, between):
    rank = gram.shape[0]
    rows = lax.broadcasted_iota(jnp.int32, (rank, rank), 0)
    cols = lax.broadcasted_iota(jnp.int32, (rank, rank), 1)
    left = gram
    right = (rows == cols).astype(F32)
    row_id = lax.broadcasted_iota(jnp.int32, (rank, 1), 0)
    for i in range(rank - 1):
        scale = 1.0 / left[i : i + 1, i : i + 1]
        col = jnp.where(row_id > i, left[:, i : i + 1], 0.0)
        row_l = left[i : i + 1, :] * scale
        row_r = right[i : i + 1, :] * scale
        left = left - col * row_l
        right = right - col * row_r
        if i % 8 == 7:
            between(i // 8)
    pivots = jnp.sum(jnp.where(rows == cols, left, 0.0), axis=1, keepdims=True)
    return right * (1.0 / jnp.sqrt(pivots))


def kernel(dims, tok_hbm, gh_hbm, rt_hbm, gt_hbm, w_hbm, err_hbm, q_hbm,
           gt_out, merged, bt_v, q_out,
           tok_all, gh_raw, gh_sel, gh_all, rt_v, gt_v, gate_sel, gate_all, w_all, x_all, gp_all,
           err_v, merged_b, back, ret, q_v, q2, facc, fbuf, rsbuf, agbuf, tbuf,
           hop_s, in_s, tok_s, tok_r, gh_s, gh_r, gate_s, gate_r, w_s, w_r,
           f_s, f_r, a_s, a_r, t_s, t_r, t_x, b_s, b_r):
    E, N, rp, chunk, gather_w, C, CB = dims
    z = lax.axis_index("expert")
    me = lax.axis_index("dp")
    tokens, width = tok_hbm.shape
    shard = width // N
    rank = q_hbm.shape[0]
    groups = width // 128
    part = tokens // C
    back_part = tokens // CB

    def other(axis, size, k):
        return lax.rem(lax.axis_index(axis) + k, size)

    def loop(size, fn, start=1):
        def step(k, c):
            fn(k)
            return c
        lax.fori_loop(start, size, step, 0)

    barrier = pltpu.get_barrier_semaphore()
    stepped = E == len(PLAN) * 2 and N & (N - 1) == 0 and N.bit_length() <= E
    bits = [1 << b for b in range(N.bit_length() - 1)]

    def greet(sem):
        for dirn in (1, -1):
            @pl.when((z + dirn >= 0) & (z + dirn < E))
            def _():
                pl.semaphore_signal(sem, inc=1, device_id={"expert": z + dirn}, device_id_type=MESH)
        for bit in bits:
            pl.semaphore_signal(sem, inc=1, device_id={"dp": me + bit - 2 * bit * lax.rem(me // bit, 2)},
                                device_id_type=MESH)

    greeted = jnp.where((z == 0) | (z == E - 1), 1, 2) + len(bits)
    if stepped:
        greet(barrier)
    else:
        for axis, size in (("expert", E), ("dp", N)):
            for k in range(1, size):
                pl.semaphore_signal(barrier, inc=1, device_id={axis: other(axis, size, k)},
                                    device_id_type=MESH)

    def w_rows(slot):
        return w_all.at[pl.ds(pl.multiple_of(slot * shard, 16), shard)] if gather_w else w_all

    loads = [
        pltpu.make_async_copy(tok_hbm, tok_all.at[z], in_s.at[0]),
        pltpu.make_async_copy(w_hbm, w_rows(me), in_s.at[1]),
        pltpu.make_async_copy(rt_hbm, rt_v, in_s.at[2]),
        pltpu.make_async_copy(gt_hbm, gt_v, in_s.at[3]),
        pltpu.make_async_copy(gh_hbm, gh_raw, in_s.at[4]),
        pltpu.make_async_copy(q_hbm, q_v, in_s.at[5]),
        pltpu.make_async_copy(err_hbm.at[0, 0], err_v, in_s.at[6]),
    ]
    for load in loads:
        load.start()

    def rdma(src, dst, s, r, axis, peer):
        return pltpu.make_async_remote_copy(
            src_ref=src, dst_ref=dst, send_sem=s, recv_sem=r,
            device_id={axis: peer}, device_id_type=MESH)

    def gate_copy(p, slot, k):
        return rdma(gate_sel.at[p], gate_all.at[slot], gate_s, gate_r.at[slot], "expert", p)

    def gh_copy(p, slot, k):
        return rdma(gh_sel.at[p], gh_all.at[slot], gh_s, gh_r.at[slot], "expert", p)

    def rows_of(c):
        return pl.ds(pl.multiple_of(c * part, 16), part)

    def tok_copy(j, c, nb, d):
        piece = tok_all.at[j, rows_of(c)]
        return rdma(piece, piece, tok_s.at[d, j], tok_r.at[j, c], "expert", nb)

    def w_copy(p, slot, k):
        return rdma(w_rows(slot), w_rows(slot), w_s, w_r.at[slot], "dp", p)

    def each(p_axis, size, copy, act):
        mine = lax.axis_index(p_axis)

        def fn(k):
            p = other(p_axis, size, k)
            if act == "start":
                copy(p, mine, k).start()
            elif act == "recv":
                copy(p, p, k).wait_recv()
            else:
                copy(p, mine, k).wait_send()
        loop(size, fn)

    partner = me + 1 - 2 * lax.rem(me, 2)
    half = N // 2
    paired = N & (N - 1) == 0

    def cross(k):
        return me + 2 * (lax.bitwise_xor(me // 2, k) - me // 2)

    loads[0].wait()
    pl.semaphore_wait(barrier, greeted if stepped else E - 1 + N - 1)

    for d, dirn in enumerate((1, -1)):
        nb = z + dirn

        @pl.when((nb >= 0) & (nb < E))
        def _():
            loop(C, lambda c: tok_copy(z, c, nb, d).start(), 0)
    for i in range(1, 4):
        loads[i].wait()
    if gather_w:
        for k in range(1, half):
            if not stepped or k in bits:
                w_copy(cross(k), me, k).start()
        w_copy(partner, me, 0).start()
    if stepped:
        greet(hop_s.at[0])

    routes = rt_v[...]
    gates = gt_v[...]

    def pick_gate(e):
        row = jnp.where(routes[0:1] == e, gates[0:1], jnp.where(routes[1:2] == e, gates[1:2], 0.0))
        gate_sel[e] = jnp.broadcast_to(row, (8, tokens))
    loop(E, pick_gate, 0)
    gate_all[z] = gate_sel[z]

    loads[4].wait()
    pairs = gh_raw[...].reshape(2 * tokens, gh_raw.shape[2])
    named = jnp.transpose(jnp.concatenate([routes.astype(F32)] * 4, axis=0))
    t_id = lax.broadcasted_iota(jnp.int32, (tokens, 2 * tokens), 0)
    p_id = lax.broadcasted_iota(jnp.int32, (tokens, 2 * tokens), 1)
    wanted = jnp.where(p_id == 2 * t_id, named[:, 0:1],
                       jnp.where(p_id == 2 * t_id + 1, named[:, 1:2], -1.0))

    def pick_rows(e):
        choose = jnp.where(wanted == e.astype(F32), 1.0, 0.0).astype(BF16)
        gh_sel[e] = jnp.dot(choose, pairs, preferred_element_type=F32).astype(BF16)

    def gh_send(p):
        gh_copy(p, z, lax.rem(p - z + E, E)).start()

    loop(E, pick_rows, 0)
    gh_all[z] = gh_sel[z]

    def mirrored(value):
        return jnp.where(z < E - 1 - z, value, E - 1 - value)

    def act(op):
        kind = op[0]
        if kind == "g":
            gh_send(mirrored(op[1]))
        elif kind == "w":
            tok_copy(mirrored(op[1]), op[2], z, 0).wait_recv()
        elif kind == "r":
            dirn = jnp.where(z < E - 1 - z, op[1], -op[1])
            tok_copy(mirrored(op[2]), op[3], z + dirn, jnp.where(dirn > 0, 0, 1)).start()
        elif kind == "x":
            pass_on(mirrored(op[1]), op[2])
        elif gather_w:
            weights()

    def acts(pick):
        for low in range(E // 2):
            @pl.when((z == low) | (z == E - 1 - low))
            def _():
                pick(low)

    def look(table, k):
        code = table[0]
        for n in range(1, len(table)):
            code = jnp.where(k == n, table[n], code)
        return code

    if stepped:
        pl.semaphore_wait(hop_s.at[0], greeted)
        for n in range(1, max(E - 2, len(bits) - 1)):
            greet(hop_s.at[n])

    loads[5].wait()
    loads[6].wait()
    q2[...] = halves(q_v[...])

    def err_factor(c):
        cols = pl.ds(pl.multiple_of(c * chunk, chunk), chunk)
        facc[:, cols] = fold(lax.dot_general(
            q2[...], err_v[cols, :], NT, preferred_element_type=F32))
    loop(width // chunk, err_factor, 0)
    if stepped:
        for n in range(1, max(E - 2, len(bits) - 1)):
            pl.semaphore_wait(hop_s.at[n], greeted)
        if gather_w:
            for k in range(1, half):
                if k not in bits:
                    w_copy(cross(k), me, k).start()
    each("expert", E, gate_copy, "start")
    if E == len(PLAN) * 2:
        acts(lambda low: [act(op) for op in PLAN[low][0]])
    else:
        loop(E, lambda k: gh_send(other("expert", E, k)))


    def back_rows(c):
        return pl.ds(pl.multiple_of(c * back_part, 16), back_part)

    def back_copy(dest, c):
        dirn = jnp.where(dest > z, 1, -1)
        nb = z + dirn
        slot = jnp.where((dest == nb) & (dest < z), E, dest)
        return rdma(back.at[dest, back_rows(c)], ret.at[slot, back_rows(c)],
                    b_s.at[dest], b_r.at[slot, c], "expert", nb)

    def back_wait(slot, c):
        rdma(back.at[0, back_rows(c)], ret.at[slot, back_rows(c)], b_s.at[0], b_r.at[slot, c],
             "expert", other("expert", E, 1)).wait_recv()

    def add_back(dest, slot, c):
        rows = back_rows(c)
        back[dest, rows, :] = (back[dest, rows, :].astype(F32)
                               + ret[slot, rows, :].astype(F32)).astype(BF16)

    def pass_on(dest, piece):
        back_wait(dest, piece)
        add_back(dest, dest, piece)
        back_copy(dest, piece).start()

    unit = tokens // 2

    def unit_rows(h):
        return pl.ds(pl.multiple_of(h * unit, 16), unit)

    def gate_column(j, h):
        column = jnp.transpose(gate_all[j])[:, :1]
        return jnp.where(h == 0, column[:unit], column[unit:])

    def inward(j, h, fresh):
        @pl.when((j != z) & fresh)
        def _():
            gate_copy(j, j, 0).wait_recv()
            gh_copy(j, j, 0).wait_recv()
        rows = unit_rows(h)
        x = (tok_all[j, rows, :].astype(F32) * gate_column(j, h)).astype(BF16)
        x_all[j, rows, :] = x
        pre = jnp.dot(x, w_all[...], preferred_element_type=F32)
        gp = (gh_all[j, rows, :].astype(F32) * slopes(pre)).astype(BF16)
        gp_all[j, rows, :] = gp
        seen = fold(lax.dot_general(q2[...], gp, NT, preferred_element_type=F32))
        facc[...] += fold(jnp.dot(halves(seen), x, preferred_element_type=F32))

    def outward(j, h):
        rows = unit_rows(h)
        back[j, rows, :] = (lax.dot_general(gp_all[j, rows, :], w_all[...], NT,
                                            preferred_element_type=F32)
                            * gate_column(j, h)).astype(BF16)

        @pl.when(((j > z) & (z == 0)) | ((j < z) & (z == E - 1)))
        def _():
            loop(CB // 2, lambda c: back_copy(j, h * (CB // 2) + c).start(), 0)

    def forward(s):
        def piece(c):
            for d, dirn in enumerate((1, -1)):
                j = z - dirn * s
                nb = z + dirn

                @pl.when((j >= 0) & (j < E))
                def _():
                    tok_copy(j, c, z, d).wait_recv()

                    @pl.when((nb >= 0) & (nb < E))
                    def _():
                        tok_copy(j, c, nb, d).start()
        loop(C, piece, 0)

    def weights():
        def pass_on(k):
            w_copy(cross(k), cross(k), 0).wait_recv()
            w_copy(partner, cross(k), half + k).start()
        loop(half, pass_on)
        w_copy(partner, partner, 0).wait_recv()
        loop(half, lambda k: w_copy(partner, partner + cross(k) - me, 0).wait_recv())

    if E == len(PLAN) * 2:
        turns = len(PLAN[0]) - 1

        def unit_at(k):
            codes = [[4 * op[1] + 2 * op[2] + op[3] for op in (turn[-1] for turn in side[1:])]
                     for side in PLAN]
            code = jnp.where((z == 0) | (z == E - 1), look(codes[0], k), look(codes[1], k))
            return mirrored(code // 4), lax.rem(code // 2, 2), lax.rem(code, 2) == 1

        def turn(k):
            def moves(low):
                for n in range(turns):
                    ops = PLAN[low][n + 1][:-1]
                    if ops:
                        @pl.when(k == n)
                        def _():
                            for op in ops:
                                act(op)
            acts(moves)
            j, h, fresh = unit_at(k)
            inward(j, h, fresh)

            @pl.when(k < turns - 1)
            def _():
                outward(j, h)
        loop(turns, turn, 0)
    else:
        def step(s):
            forward(s)
            if gather_w:
                @pl.when(s == 1)
                def _():
                    weights()

            def block(i, carry):
                side = i // 2
                h = lax.rem(i, 2)
                j = jnp.where(side == 0, z, jnp.where(side == 1, z - s, z + s))

                @pl.when((j >= 0) & (j < E) & ((side > 0) | (s == 1)))
                def _():
                    inward(j, h, h == 0)
                    outward(j, h)
                return carry
            lax.fori_loop(0, 6, block, 0)
        loop(E, step)

    if fbuf.shape[0] > groups * rank:
        fbuf[groups * rank :, :] = jnp.zeros((fbuf.shape[0] - groups * rank, 128), BF16)
    for c in range(groups):
        fbuf[c * rank : (c + 1) * rank, :] = facc[:, c * 128 : (c + 1) * 128].astype(BF16)

    def f_copy(p, slot, k):
        return rdma(fbuf.at[pl.ds(pl.multiple_of(p * rp, 16), rp)], rsbuf.at[slot],
                    f_s, f_r, "dp", p)

    def a_copy(p, slot, k):
        piece = agbuf.at[pl.ds(pl.multiple_of(slot * rp, 16), rp)]
        return rdma(piece, piece, a_s, a_r, "dp", p)

    def t_copy(p, slot, sem):
        return rdma(tbuf.at[slot], tbuf.at[slot], t_s, sem, "dp", p)

    def all_f():
        return rdma(rsbuf.at[pl.ds(0, N - 1)], rsbuf.at[pl.ds(0, N - 1)], f_s, f_r, "dp", partner)

    def all_a():
        rest = agbuf.at[pl.ds(0, rp * (N - 1))]
        return rdma(rest, rest, a_s, a_r, "dp", partner)

    def all_t(count, sem):
        slots = tbuf.at[pl.ds(0, count)]
        return rdma(slots, slots, t_s, sem, "dp", partner)

    own = pl.ds(pl.multiple_of(me * rp, 16), rp)
    each("dp", N, f_copy, "start")
    rsbuf[me] = fbuf[own, :]

    if E == len(PLAN) * 2:
        j, h, _ = unit_at(turns - 1)
        outward(j, h)

    right_first = z < E - 1 - z
    lag = 3

    def relay(m, c):
        def turn(i, carry):
            right = (i == 0) == right_first
            dest = jnp.where(right, m, E - 1 - m)
            hop = jnp.where(right, (dest > z) & (z > 0), (dest < z) & (z < E - 1))
            piece = c - lag * i

            @pl.when(hop & (piece >= 0) & (piece < CB))
            def _():
                back_wait(dest, piece)
                add_back(dest, dest, piece)
                back_copy(dest, piece).start()
            return carry
        lax.fori_loop(0, 2, turn, 0)

    def planned(start, stop):
        @pl.when((z > 0) & (z < E - 1))
        def _():
            def one(i, carry):
                code = look([CB * op[0] + op[1] for op in RELAYS], i)
                pass_on(mirrored(code // CB), lax.rem(code, CB))
                return carry
            lax.fori_loop(start, stop, one, 0)

    def relays(start, stop, first, last):
        def rank_of(m, carry):
            loop(last, lambda c: relay(m, c), first)
            return carry
        lax.fori_loop(start, stop, rank_of, 0)

    def merge(c):
        cols = pl.ds(pl.multiple_of(c * chunk, chunk), chunk)
        x = x_all[:, :, cols].reshape(E * tokens, chunk)
        gp = gp_all[...].reshape(E * tokens, gp_all.shape[2])
        m = lax.dot_general(x, gp, TN, preferred_element_type=F32)
        m = m + err_v[cols, :].astype(F32)
        merged[cols, :] = m
        merged_b[cols, :] = m.astype(BF16)
    if E == len(PLAN) * 2:
        planned(0, STOPS[0])
    else:
        relays(1, E - 1, 0, CB // 2)
    all_f().wait_recv()
    agbuf[own, :] = (jnp.sum(rsbuf[...].astype(F32), axis=0) * (1.0 / N)).astype(BF16)
    each("dp", N, a_copy, "start")
    loop(width // chunk, merge, 0)

    if E == len(PLAN) * 2:
        planned(STOPS[0], STOPS[1])
    else:
        relays(1, E - 1, CB // 2, CB + lag)
    all_a().wait_recv()
    factor = jnp.concatenate([agbuf[c * rank : (c + 1) * rank, :] for c in range(groups)], axis=1)
    tbuf[me] = jnp.dot(factor, merged_b[...], preferred_element_type=F32).astype(BF16)
    if paired:
        loop(half, lambda k: t_copy(cross(k), me, t_x).start())
        t_copy(partner, me, t_r).start()
    else:
        loop(N, lambda k: t_copy(other("dp", N, k), me, t_r).start())

    if E == len(PLAN) * 2:
        planned(STOPS[1], STOPS[2])
    gram = lax.dot_general(factor, factor, NT, preferred_element_type=F32)
    def between(n):
        if E == len(PLAN) * 2 and n + 3 < len(STOPS):
            planned(STOPS[n + 2], STOPS[n + 3])
    inverse = inverse_factor(gram, between)
    basis = fold(jnp.dot(halves(inverse), factor, preferred_element_type=F32))
    bt_v[...] = jnp.transpose(basis).astype(BF16)
    if paired:
        all_t(half - 1, t_x).wait_recv()
        loop(half, lambda k: t_copy(partner, cross(k), t_r).start())

    if E == len(PLAN) * 2:
        planned(STOPS[-1], len(RELAYS))
    else:
        relays(E - 1, E, 0, CB + lag)
    for d, dirn in enumerate((1, -1)):
        nb = z + dirn
        ahead = z if d == 0 else E - 1 - z

        @pl.when((nb >= 0) & (nb < E))
        def _():
            def drain(s):
                @pl.when(s <= ahead)
                def _():
                    j = z - dirn * s
                    rdma(tok_all.at[j], tok_all.at[j], tok_s.at[d, j], tok_r.at[j, 0],
                         "expert", nb).wait_send()
            loop(E, drain, 0)
    rdma(gate_sel.at[pl.ds(0, E - 1)], gate_all.at[pl.ds(0, E - 1)], gate_s, gate_r.at[0],
         "expert", other("expert", E, 1)).wait_send()
    rdma(gh_sel.at[pl.ds(0, E - 1)], gh_all.at[pl.ds(0, E - 1)], gh_s, gh_r.at[0],
         "expert", other("expert", E, 1)).wait_send()
    if gather_w:
        rest = w_all.at[pl.ds(0, shard * (N - 1))]
        rdma(rest, rest, w_s, w_r.at[0], "dp", partner).wait_send()
    all_f().wait_send()
    all_a().wait_send()
    all_t(half if paired else N - 1, t_r).wait_recv()
    mean = jnp.sum(tbuf[...].astype(F32), axis=0) * (1.0 / N)
    q_out[...] = jnp.dot(inverse, mean, precision=HI, preferred_element_type=F32).astype(BF16)

    @pl.when(z > 0)
    def _():
        def piece(c):
            back_wait(z, c)
            add_back(z, z, c)
        loop(CB, piece, 0)

    @pl.when(z < E - 1)
    def _():
        def piece(c):
            back_wait(E, c)
            add_back(z, E, c)
        loop(CB, piece, 0)
    gt_out[...] = back[z]

    def sent(k):
        dest = other("expert", E, k)
        rdma(back.at[dest], ret.at[dest], b_s.at[dest], b_r.at[dest, 0], "expert",
             other("expert", E, 1)).wait_send()
    loop(E, sent)
    all_t(N - 1, t_s).wait_send()


def finish(chunk, gt_v, merged, bt_v, q_v, gt_hbm, err_hbm, wg_hbm, err_v, wg_v, sem):
    width = merged.shape[0]
    shard = wg_v.shape[0]
    me = lax.axis_index("dp")
    count = width // chunk
    moves = [pltpu.make_async_copy(gt_v, gt_hbm, sem.at[0])]
    moves[0].start()
    wg_v[...] = jnp.dot(bt_v[pl.ds(pl.multiple_of(me * shard, 8), shard), :], q_v[...],
                        preferred_element_type=F32)
    moves.append(pltpu.make_async_copy(wg_v, wg_hbm.at[0], sem.at[1]))
    moves[1].start()
    for c in range(count):
        rows = pl.ds(c * chunk, chunk)
        low = jnp.dot(bt_v[rows, :], q_v[...], preferred_element_type=F32)
        err_v[rows, :] = (merged[rows, :] - low).astype(BF16)
        moves.append(pltpu.make_async_copy(err_v.at[rows], err_hbm.at[0, 0, rows], sem.at[2 + c]))
        moves[-1].start()
    for move in moves:
        move.wait()


def body(tokens, routes, gates, grad_hidden, w_in, error, q_seed):
    E = lax.axis_size("expert")
    N = lax.axis_size("dp")
    rows, width = tokens.shape
    hidden = grad_hidden.shape[2]
    rank = q_seed.shape[2]
    shard = width // N
    gather_w = shard % 16 == 0 and N & (N - 1) == 0
    weight = w_in[0] if gather_w else lax.all_gather(w_in[0], "dp", axis=0, tiled=True)
    chunk = 256 if width % 256 == 0 else 128
    C, CB = (4, 8) if E <= 8 else (2, 2)
    room = (4 * E + 3) * rows * width * 2 + 3 * E * rows * hidden * 2 + 13 * width * hidden + (12 << 20)
    total_rows = width // 128 * rank
    rp = -(-total_rows // N)
    rp = -(-rp // 16) * 16
    dma = pltpu.SemaphoreType.DMA
    vmem = pl.BlockSpec(memory_space=pltpu.VMEM)
    hbm = pl.BlockSpec(memory_space=pltpu.HBM)
    parts = pl.pallas_call(
        functools.partial(kernel, (E, N, rp, chunk, gather_w, C, CB)),
        out_shape=(
            jax.ShapeDtypeStruct((rows, width), BF16),
            jax.ShapeDtypeStruct((width, hidden), F32),
            jax.ShapeDtypeStruct((width, rank), BF16),
            jax.ShapeDtypeStruct((rank, hidden), BF16),
        ),
        in_specs=[hbm] * 7,
        out_specs=(vmem,) * 4,
        scratch_shapes=[
            pltpu.VMEM((E, rows, width), BF16),
            pltpu.VMEM((rows, 2, hidden), BF16),
            pltpu.VMEM((E, rows, hidden), BF16),
            pltpu.VMEM((E, rows, hidden), BF16),
            pltpu.VMEM((2, rows), jnp.int32),
            pltpu.VMEM((2, rows), F32),
            pltpu.VMEM((E, 8, rows), F32),
            pltpu.VMEM((E, 8, rows), F32),
            pltpu.VMEM((width, hidden), BF16),
            pltpu.VMEM((E, rows, width), BF16),
            pltpu.VMEM((E, rows, hidden), BF16),
            pltpu.VMEM((width, hidden), BF16),
            pltpu.VMEM((width, hidden), BF16),
            pltpu.VMEM((E, rows, width), BF16),
            pltpu.VMEM((E + 1, rows, width), BF16),
            pltpu.VMEM((rank, hidden), F32),
            pltpu.VMEM((2 * rank, hidden), BF16),
            pltpu.VMEM((rank, width), F32),
            pltpu.VMEM((rp * N, 128), BF16),
            pltpu.VMEM((N, rp, 128), BF16),
            pltpu.VMEM((rp * N, 128), BF16),
            pltpu.VMEM((N, rank, hidden), BF16),
            pltpu.SemaphoreType.REGULAR((2,)), dma((7,)), dma((2, E)), dma((E, C)), dma(()), dma((E,)), dma(()), dma((E,)),
            dma(()), dma((N,)), dma(()), dma(()), dma(()), dma(()), dma(()), dma(()),
            dma(()), dma((E,)), dma((E + 1, CB)),
        ],
        compiler_params=pltpu.CompilerParams(
            collective_id=0, has_side_effects=True, vmem_limit_bytes=min(room, 67043328 - (1 << 20))),
    )(*(pltpu.with_memory_space_constraint(a, pltpu.HBM) for a in (
        tokens, grad_hidden, routes.T, gates.T, weight, error, q_seed[0].T)))
    return pl.pallas_call(
        functools.partial(finish, chunk),
        out_shape=(
            jax.ShapeDtypeStruct((rows, width), BF16),
            jax.ShapeDtypeStruct((1, 1, width, hidden), BF16),
            jax.ShapeDtypeStruct((1, shard, hidden), F32),
        ),
        in_specs=[vmem] * 4,
        out_specs=(hbm, hbm, hbm),
        scratch_shapes=[
            pltpu.VMEM((width, hidden), BF16),
            pltpu.VMEM((shard, hidden), F32),
            dma((2 + width // chunk,)),
        ],
        compiler_params=pltpu.CompilerParams(vmem_limit_bytes=16 << 20),
    )(*parts)


def solution(mesh):
    placed = (
        P(("dp", "expert"), None),
        P(("dp", "expert"), None),
        P(("dp", "expert"), None),
        P(("dp", "expert"), None, None),
        P("expert", "dp", None),
        P("dp", "expert", None, None),
        P("expert", None, None),
    )
    return jax.shard_map(
        body,
        mesh=mesh,
        in_specs=placed,
        out_specs=(
            P(("dp", "expert"), None),
            P("dp", "expert", None, None),
            P("expert", "dp", None),
        ),
        check_vma=False,
    )
```

```python
import functools

import jax
import jax.numpy as jnp
from jax import lax
from jax.experimental import pallas as pl
from jax.experimental.pallas import tpu as pltpu
from jax.sharding import PartitionSpec as P

HI = lax.Precision.HIGHEST
MESH = pl.DeviceIdType.MESH
F32 = jnp.float32
BF16 = jnp.bfloat16
NT = (((1,), (1,)), ((), ()))
TN = (((0,), (0,)), ((), ()))


PLAN = (
    (
        (("g", 1), ("g", 2), ("g", 3),),
        (("w", 1, 0), ("w", 1, 1), ("w", 1, 2), ("w", 1, 3), ("W",), ("u", 1, 0, 1),),
        (("u", 1, 1, 0),),
        (("u", 0, 0, 1),),
        (("u", 0, 1, 0),),
        (("w", 2, 0), ("w", 2, 1), ("u", 2, 0, 1),),
        (("w", 3, 0), ("w", 3, 1), ("u", 3, 0, 1),),
        (("w", 3, 2), ("w", 3, 3), ("u", 3, 1, 0),),
        (("w", 2, 2), ("w", 2, 3), ("u", 2, 1, 0),),
    ),
    (
        (("g", 0), ("g", 2), ("g", 3),),
        (("w", 0, 0), ("r", 1, 0, 0), ("w", 2, 0), ("r", -1, 2, 0), ("w", 0, 1), ("r", 1, 0, 1), ("w", 2, 1), ("r", -1, 2, 1), ("w", 0, 2), ("r", 1, 0, 2), ("w", 2, 2), ("r", -1, 2, 2), ("w", 0, 3), ("r", 1, 0, 3), ("w", 2, 3), ("W",), ("u", 1, 0, 1),),
        (("u", 1, 1, 0),),
        (("u", 0, 0, 1),),
        (("u", 0, 1, 0),),
        (("u", 2, 0, 1),),
        (("u", 2, 1, 0),),
        (("w", 3, 0), ("r", -1, 3, 0), ("w", 3, 1), ("r", -1, 3, 1), ("u", 3, 0, 1),),
        (("w", 3, 2), ("r", -1, 3, 2), ("w", 3, 3), ("r", -1, 3, 3), ("r", -1, 2, 3), ("u", 3, 1, 0),),
    ),
)
RELAYS = (
    (2, 0), (2, 1), (2, 2), (2, 3), (3, 0), (3, 1), (3, 2), (3, 3),
    (0, 0), (3, 4), (0, 1), (3, 5), (0, 2), (3, 6), (0, 3), (3, 7),
    (0, 4), (2, 4), (0, 5), (2, 5), (0, 6), (2, 6), (0, 7), (2, 7),
)
STOPS = (4, 7, 8, 10, 12, 14)


def slopes(pre_act):
    squashed = 1.0 / (1.0 + jnp.exp(-pre_act))
    return squashed * (1.0 + pre_act * (1.0 - squashed))


def halves(value):
    high = value.astype(BF16)
    low = (value - high.astype(F32)).astype(BF16)
    return jnp.concatenate([high, low], axis=0)


def fold(value):
    rows = value.shape[0] // 2
    return value[:rows] + value[rows:]


def inverse_factor(gram, between):
    rank = gram.shape[0]
    rows = lax.broadcasted_iota(jnp.int32, (rank, rank), 0)
    cols = lax.broadcasted_iota(jnp.int32, (rank, rank), 1)
    left = gram
    right = (rows == cols).astype(F32)
    row_id = lax.broadcasted_iota(jnp.int32, (rank, 1), 0)
    for i in range(rank - 1):
        scale = 1.0 / left[i : i + 1, i : i + 1]
        col = jnp.where(row_id > i, left[:, i : i + 1], 0.0)
        row_l = left[i : i + 1, :] * scale
        row_r = right[i : i + 1, :] * scale
        left = left - col * row_l
        right = right - col * row_r
        if i % 8 == 7:
            between(i // 8)
    pivots = jnp.sum(jnp.where(rows == cols, left, 0.0), axis=1, keepdims=True)
    return right * (1.0 / jnp.sqrt(pivots))


def kernel(dims, tok_hbm, gh_hbm, rt_hbm, gt_hbm, w_hbm, err_hbm, q_hbm,
           gt_out, merged, bt_v, q_out,
           tok_all, gh_raw, gh_sel, gh_all, rt_v, gt_v, gate_sel, gate_all, w_all, x_all, gp_all,
           err_v, merged_b, back, ret, q_v, q2, facc, fbuf, rsbuf, agbuf, tbuf,
           hop_s, in_s, tok_s, tok_r, gh_s, gh_r, gate_s, gate_r, w_s, w_r,
           f_s, f_r, a_s, a_r, t_s, t_r, t_x, b_s, b_r):
    E, N, rp, chunk, gather_w, C, CB = dims
    z = lax.axis_index("expert")
    me = lax.axis_index("dp")
    tokens, width = tok_hbm.shape
    shard = width // N
    rank = q_hbm.shape[0]
    groups = width // 128
    part = tokens // C
    paired = N & (N - 1) == 0
    back_part = tokens // CB

    def other(axis, size, k):
        return lax.rem(lax.axis_index(axis) + k, size)

    def loop(size, fn, start=1):
        def step(k, c):
            fn(k)
            return c
        lax.fori_loop(start, size, step, 0)

    barrier = pltpu.get_barrier_semaphore()
    stepped = E == len(PLAN) * 2 and N & (N - 1) == 0 and N.bit_length() <= E
    bits = [1 << b for b in range(N.bit_length() - 1)]

    def spread(copy):
        if paired:
            for k in sorted(range(1, N), key=lambda k: (-(k // 2).bit_count(), -k)):
                copy(lax.bitwise_xor(me, k), me, k).start()
        else:
            each("dp", N, copy, "start")

    def greet(sem):
        for dirn in (1, -1):
            @pl.when((z + dirn >= 0) & (z + dirn < E))
            def _():
                pl.semaphore_signal(sem, inc=1, device_id={"expert": z + dirn}, device_id_type=MESH)
        for bit in bits:
            pl.semaphore_signal(sem, inc=1, device_id={"dp": me + bit - 2 * bit * lax.rem(me // bit, 2)},
                                device_id_type=MESH)

    greeted = jnp.where((z == 0) | (z == E - 1), 1, 2) + len(bits)
    if stepped:
        greet(barrier)
    else:
        for axis, size in (("expert", E), ("dp", N)):
            for k in range(1, size):
                pl.semaphore_signal(barrier, inc=1, device_id={axis: other(axis, size, k)},
                                    device_id_type=MESH)

    def w_rows(slot):
        return w_all.at[pl.ds(pl.multiple_of(slot * shard, 16), shard)] if gather_w else w_all

    loads = [
        pltpu.make_async_copy(tok_hbm, tok_all.at[z], in_s.at[0]),
        pltpu.make_async_copy(w_hbm, w_rows(me), in_s.at[1]),
        pltpu.make_async_copy(rt_hbm, rt_v, in_s.at[2]),
        pltpu.make_async_copy(gt_hbm, gt_v, in_s.at[3]),
        pltpu.make_async_copy(gh_hbm, gh_raw, in_s.at[4]),
        pltpu.make_async_copy(q_hbm, q_v, in_s.at[5]),
        pltpu.make_async_copy(err_hbm.at[0, 0], err_v, in_s.at[6]),
    ]
    for load in loads:
        load.start()

    def rdma(src, dst, s, r, axis, peer):
        return pltpu.make_async_remote_copy(
            src_ref=src, dst_ref=dst, send_sem=s, recv_sem=r,
            device_id={axis: peer}, device_id_type=MESH)

    def gate_copy(p, slot, k):
        return rdma(gate_sel.at[p], gate_all.at[slot], gate_s, gate_r.at[slot], "expert", p)

    def gh_copy(p, slot, k):
        return rdma(gh_sel.at[p], gh_all.at[slot], gh_s, gh_r.at[slot], "expert", p)

    def rows_of(c):
        return pl.ds(pl.multiple_of(c * part, 16), part)

    def tok_copy(j, c, nb, d):
        piece = tok_all.at[j, rows_of(c)]
        return rdma(piece, piece, tok_s.at[d, j], tok_r.at[j, c], "expert", nb)

    def w_copy(p, slot, k):
        return rdma(w_rows(slot), w_rows(slot), w_s, w_r.at[slot], "dp", p)

    def each(p_axis, size, copy, act):
        mine = lax.axis_index(p_axis)

        def fn(k):
            p = other(p_axis, size, k)
            if act == "start":
                copy(p, mine, k).start()
            elif act == "recv":
                copy(p, p, k).wait_recv()
            else:
                copy(p, mine, k).wait_send()
        loop(size, fn)

    partner = me + 1 - 2 * lax.rem(me, 2)
    half = N // 2

    def cross(k):
        return me + 2 * (lax.bitwise_xor(me // 2, k) - me // 2)

    loads[0].wait()
    pl.semaphore_wait(barrier, greeted if stepped else E - 1 + N - 1)

    for d, dirn in enumerate((1, -1)):
        nb = z + dirn

        @pl.when((nb >= 0) & (nb < E))
        def _():
            loop(C, lambda c: tok_copy(z, c, nb, d).start(), 0)
    for i in range(1, 4):
        loads[i].wait()
    if gather_w:
        for k in range(1, half):
            if not stepped or k in bits:
                w_copy(cross(k), me, k).start()
        w_copy(partner, me, 0).start()
    if stepped:
        greet(hop_s.at[0])

    routes = rt_v[...]
    gates = gt_v[...]

    def pick_gate(e):
        row = jnp.where(routes[0:1] == e, gates[0:1], jnp.where(routes[1:2] == e, gates[1:2], 0.0))
        gate_sel[e] = jnp.broadcast_to(row, (8, tokens))
    loop(E, pick_gate, 0)
    gate_all[z] = gate_sel[z]

    loads[4].wait()
    pairs = gh_raw[...].reshape(2 * tokens, gh_raw.shape[2])
    named = jnp.transpose(jnp.concatenate([routes.astype(F32)] * 4, axis=0))
    t_id = lax.broadcasted_iota(jnp.int32, (tokens, 2 * tokens), 0)
    p_id = lax.broadcasted_iota(jnp.int32, (tokens, 2 * tokens), 1)
    wanted = jnp.where(p_id == 2 * t_id, named[:, 0:1],
                       jnp.where(p_id == 2 * t_id + 1, named[:, 1:2], -1.0))

    def pick_rows(e):
        choose = jnp.where(wanted == e.astype(F32), 1.0, 0.0).astype(BF16)
        gh_sel[e] = jnp.dot(choose, pairs, preferred_element_type=F32).astype(BF16)

    def gh_send(p):
        gh_copy(p, z, lax.rem(p - z + E, E)).start()

    loop(E, pick_rows, 0)
    gh_all[z] = gh_sel[z]

    def mirrored(value):
        return jnp.where(z < E - 1 - z, value, E - 1 - value)

    def act(op):
        kind = op[0]
        if kind == "g":
            gh_send(mirrored(op[1]))
        elif kind == "w":
            tok_copy(mirrored(op[1]), op[2], z, 0).wait_recv()
        elif kind == "r":
            dirn = jnp.where(z < E - 1 - z, op[1], -op[1])
            tok_copy(mirrored(op[2]), op[3], z + dirn, jnp.where(dirn > 0, 0, 1)).start()
        elif kind == "x":
            pass_on(mirrored(op[1]), op[2])
        elif gather_w:
            weights()

    def acts(pick):
        for low in range(E // 2):
            @pl.when((z == low) | (z == E - 1 - low))
            def _():
                pick(low)

    def look(table, k):
        code = table[0]
        for n in range(1, len(table)):
            code = jnp.where(k == n, table[n], code)
        return code

    if stepped:
        pl.semaphore_wait(hop_s.at[0], greeted)
        for n in range(1, max(E - 2, len(bits) - 1)):
            greet(hop_s.at[n])

    loads[5].wait()
    loads[6].wait()
    q2[...] = halves(q_v[...])

    def err_factor(c):
        cols = pl.ds(pl.multiple_of(c * chunk, chunk), chunk)
        facc[:, cols] = fold(lax.dot_general(
            q2[...], err_v[cols, :], NT, preferred_element_type=F32))
    loop(width // chunk, err_factor, 0)
    if stepped:
        for n in range(1, max(E - 2, len(bits) - 1)):
            pl.semaphore_wait(hop_s.at[n], greeted)
        if gather_w:
            for k in range(1, half):
                if k not in bits:
                    w_copy(cross(k), me, k).start()
    each("expert", E, gate_copy, "start")
    if E == len(PLAN) * 2:
        acts(lambda low: [act(op) for op in PLAN[low][0]])
    else:
        loop(E, lambda k: gh_send(other("expert", E, k)))


    def back_rows(c):
        return pl.ds(pl.multiple_of(c * back_part, 16), back_part)

    def back_copy(dest, c):
        dirn = jnp.where(dest > z, 1, -1)
        nb = z + dirn
        slot = jnp.where((dest == nb) & (dest < z), E, dest)
        return rdma(back.at[dest, back_rows(c)], ret.at[slot, back_rows(c)],
                    b_s.at[dest], b_r.at[slot, c], "expert", nb)

    def back_wait(slot, c):
        rdma(back.at[0, back_rows(c)], ret.at[slot, back_rows(c)], b_s.at[0], b_r.at[slot, c],
             "expert", other("expert", E, 1)).wait_recv()

    def add_back(dest, slot, c):
        rows = back_rows(c)
        back[dest, rows, :] = (back[dest, rows, :].astype(F32)
                               + ret[slot, rows, :].astype(F32)).astype(BF16)

    def pass_on(dest, piece):
        back_wait(dest, piece)
        add_back(dest, dest, piece)
        back_copy(dest, piece).start()

    unit = tokens // 2

    def unit_rows(h):
        return pl.ds(pl.multiple_of(h * unit, 16), unit)

    def gate_column(j, h):
        column = jnp.transpose(gate_all[j])[:, :1]
        return jnp.where(h == 0, column[:unit], column[unit:])

    def inward(j, h, fresh):
        @pl.when((j != z) & fresh)
        def _():
            gate_copy(j, j, 0).wait_recv()
            gh_copy(j, j, 0).wait_recv()
        rows = unit_rows(h)
        x = (tok_all[j, rows, :].astype(F32) * gate_column(j, h)).astype(BF16)
        x_all[j, rows, :] = x
        pre = jnp.dot(x, w_all[...], preferred_element_type=F32)
        gp = (gh_all[j, rows, :].astype(F32) * slopes(pre)).astype(BF16)
        gp_all[j, rows, :] = gp
        seen = fold(lax.dot_general(q2[...], gp, NT, preferred_element_type=F32))
        facc[...] += fold(jnp.dot(halves(seen), x, preferred_element_type=F32))

    def outward(j, h):
        rows = unit_rows(h)
        back[j, rows, :] = (lax.dot_general(gp_all[j, rows, :], w_all[...], NT,
                                            preferred_element_type=F32)
                            * gate_column(j, h)).astype(BF16)

        @pl.when(((j > z) & (z == 0)) | ((j < z) & (z == E - 1)))
        def _():
            loop(CB // 2, lambda c: back_copy(j, h * (CB // 2) + c).start(), 0)

    def forward(s):
        def piece(c):
            for d, dirn in enumerate((1, -1)):
                j = z - dirn * s
                nb = z + dirn

                @pl.when((j >= 0) & (j < E))
                def _():
                    tok_copy(j, c, z, d).wait_recv()

                    @pl.when((nb >= 0) & (nb < E))
                    def _():
                        tok_copy(j, c, nb, d).start()
        loop(C, piece, 0)

    def weights():
        def pass_on(k):
            w_copy(cross(k), cross(k), 0).wait_recv()
            w_copy(partner, cross(k), half + k).start()
        loop(half, pass_on)
        w_copy(partner, partner, 0).wait_recv()
        loop(half, lambda k: w_copy(partner, partner + cross(k) - me, 0).wait_recv())

    if E == len(PLAN) * 2:
        turns = len(PLAN[0]) - 1

        def unit_at(k):
            codes = [[4 * op[1] + 2 * op[2] + op[3] for op in (turn[-1] for turn in side[1:])]
                     for side in PLAN]
            code = jnp.where((z == 0) | (z == E - 1), look(codes[0], k), look(codes[1], k))
            return mirrored(code // 4), lax.rem(code // 2, 2), lax.rem(code, 2) == 1

        def turn(k):
            def moves(low):
                for n in range(turns):
                    ops = PLAN[low][n + 1][:-1]
                    if ops:
                        @pl.when(k == n)
                        def _():
                            for op in ops:
                                act(op)
            acts(moves)
            j, h, fresh = unit_at(k)
            inward(j, h, fresh)

            @pl.when(k < turns - 1)
            def _():
                outward(j, h)
        loop(turns, turn, 0)
    else:
        def step(s):
            forward(s)
            if gather_w:
                @pl.when(s == 1)
                def _():
                    weights()

            def block(i, carry):
                side = i // 2
                h = lax.rem(i, 2)
                j = jnp.where(side == 0, z, jnp.where(side == 1, z - s, z + s))

                @pl.when((j >= 0) & (j < E) & ((side > 0) | (s == 1)))
                def _():
                    inward(j, h, h == 0)
                    outward(j, h)
                return carry
            lax.fori_loop(0, 6, block, 0)
        loop(E, step)

    if fbuf.shape[0] > groups * rank:
        fbuf[groups * rank :, :] = jnp.zeros((fbuf.shape[0] - groups * rank, 128), BF16)
    for c in range(groups):
        fbuf[c * rank : (c + 1) * rank, :] = facc[:, c * 128 : (c + 1) * 128].astype(BF16)

    def f_copy(p, slot, k):
        return rdma(fbuf.at[pl.ds(pl.multiple_of(p * rp, 16), rp)], rsbuf.at[slot],
                    f_s, f_r, "dp", p)

    def a_copy(p, slot, k):
        piece = agbuf.at[pl.ds(pl.multiple_of(slot * rp, 16), rp)]
        return rdma(piece, piece, a_s, a_r, "dp", p)

    def t_copy(p, slot, sem):
        return rdma(tbuf.at[slot], tbuf.at[slot], t_s, sem, "dp", p)

    def all_f():
        return rdma(rsbuf.at[pl.ds(0, N - 1)], rsbuf.at[pl.ds(0, N - 1)], f_s, f_r, "dp", partner)

    def all_a():
        rest = agbuf.at[pl.ds(0, rp * (N - 1))]
        return rdma(rest, rest, a_s, a_r, "dp", partner)

    def all_t(count, sem):
        slots = tbuf.at[pl.ds(0, count)]
        return rdma(slots, slots, t_s, sem, "dp", partner)

    own = pl.ds(pl.multiple_of(me * rp, 16), rp)
    spread(f_copy)
    rsbuf[me] = fbuf[own, :]

    if E == len(PLAN) * 2:
        j, h, _ = unit_at(turns - 1)
        outward(j, h)

    right_first = z < E - 1 - z
    lag = 3

    def relay(m, c):
        def turn(i, carry):
            right = (i == 0) == right_first
            dest = jnp.where(right, m, E - 1 - m)
            hop = jnp.where(right, (dest > z) & (z > 0), (dest < z) & (z < E - 1))
            piece = c - lag * i

            @pl.when(hop & (piece >= 0) & (piece < CB))
            def _():
                back_wait(dest, piece)
                add_back(dest, dest, piece)
                back_copy(dest, piece).start()
            return carry
        lax.fori_loop(0, 2, turn, 0)

    def planned(start, stop):
        @pl.when((z > 0) & (z < E - 1))
        def _():
            def one(i, carry):
                code = look([CB * op[0] + op[1] for op in RELAYS], i)
                pass_on(mirrored(code // CB), lax.rem(code, CB))
                return carry
            lax.fori_loop(start, stop, one, 0)

    def relays(start, stop, first, last):
        def rank_of(m, carry):
            loop(last, lambda c: relay(m, c), first)
            return carry
        lax.fori_loop(start, stop, rank_of, 0)

    def merge(c):
        cols = pl.ds(pl.multiple_of(c * chunk, chunk), chunk)
        x = x_all[:, :, cols].reshape(E * tokens, chunk)
        gp = gp_all[...].reshape(E * tokens, gp_all.shape[2])
        m = lax.dot_general(x, gp, TN, preferred_element_type=F32)
        m = m + err_v[cols, :].astype(F32)
        merged[cols, :] = m
        merged_b[cols, :] = m.astype(BF16)
    if E == len(PLAN) * 2:
        planned(0, STOPS[0])
    else:
        relays(1, E - 1, 0, CB // 2)
    all_f().wait_recv()
    agbuf[own, :] = (jnp.sum(rsbuf[...].astype(F32), axis=0) * (1.0 / N)).astype(BF16)
    spread(a_copy)
    if E == len(PLAN) * 2:
        cut = width // chunk // 2 + 1
        planned(STOPS[0], STOPS[0] + 1)
        loop(cut, merge, 0)
        planned(STOPS[0] + 1, STOPS[0] + 2)
        loop(width // chunk, merge, cut)
    else:
        loop(width // chunk, merge, 0)

    if E == len(PLAN) * 2:
        planned(STOPS[0] + 2, STOPS[1])
    else:
        relays(1, E - 1, CB // 2, CB + lag)
    all_a().wait_recv()
    factor = jnp.concatenate([agbuf[c * rank : (c + 1) * rank, :] for c in range(groups)], axis=1)
    tbuf[me] = jnp.dot(factor, merged_b[...], preferred_element_type=F32).astype(BF16)
    if paired:
        loop(half, lambda k: t_copy(cross(k), me, t_x).start())
        t_copy(partner, me, t_r).start()
    else:
        loop(N, lambda k: t_copy(other("dp", N, k), me, t_r).start())

    if E == len(PLAN) * 2:
        planned(STOPS[1], STOPS[2])
    gram = lax.dot_general(factor, factor, NT, preferred_element_type=F32)
    def between(n):
        if E == len(PLAN) * 2 and n + 3 < len(STOPS):
            planned(STOPS[n + 2], STOPS[n + 3])
    inverse = inverse_factor(gram, between)
    basis = fold(jnp.dot(halves(inverse), factor, preferred_element_type=F32))
    bt_v[...] = jnp.transpose(basis).astype(BF16)
    if paired:
        all_t(half - 1, t_x).wait_recv()
        loop(half, lambda k: t_copy(partner, cross(k), t_r).start())

    if E == len(PLAN) * 2:
        planned(STOPS[-1], len(RELAYS))
    else:
        relays(E - 1, E, 0, CB + lag)
    for d, dirn in enumerate((1, -1)):
        nb = z + dirn
        ahead = z if d == 0 else E - 1 - z

        @pl.when((nb >= 0) & (nb < E))
        def _():
            def drain(s):
                @pl.when(s <= ahead)
                def _():
                    j = z - dirn * s
                    rdma(tok_all.at[j], tok_all.at[j], tok_s.at[d, j], tok_r.at[j, 0],
                         "expert", nb).wait_send()
            loop(E, drain, 0)
    rdma(gate_sel.at[pl.ds(0, E - 1)], gate_all.at[pl.ds(0, E - 1)], gate_s, gate_r.at[0],
         "expert", other("expert", E, 1)).wait_send()
    rdma(gh_sel.at[pl.ds(0, E - 1)], gh_all.at[pl.ds(0, E - 1)], gh_s, gh_r.at[0],
         "expert", other("expert", E, 1)).wait_send()
    if gather_w:
        rest = w_all.at[pl.ds(0, shard * (N - 1))]
        rdma(rest, rest, w_s, w_r.at[0], "dp", partner).wait_send()
    all_f().wait_send()
    all_a().wait_send()
    all_t(half if paired else N - 1, t_r).wait_recv()
    mean = jnp.sum(tbuf[...].astype(F32), axis=0) * (1.0 / N)
    q_out[...] = jnp.dot(inverse, mean, precision=HI, preferred_element_type=F32).astype(BF16)

    @pl.when(z > 0)
    def _():
        def piece(c):
            back_wait(z, c)
            add_back(z, z, c)
        loop(CB, piece, 0)

    @pl.when(z < E - 1)
    def _():
        def piece(c):
            back_wait(E, c)
            add_back(z, E, c)
        loop(CB, piece, 0)
    gt_out[...] = back[z]

    def sent(k):
        dest = other("expert", E, k)
        rdma(back.at[dest], ret.at[dest], b_s.at[dest], b_r.at[dest, 0], "expert",
             other("expert", E, 1)).wait_send()
    loop(E, sent)
    all_t(N - 1, t_s).wait_send()


def finish(chunk, gt_v, merged, bt_v, q_v, gt_hbm, err_hbm, wg_hbm, err_v, wg_v, sem):
    width = merged.shape[0]
    shard = wg_v.shape[0]
    me = lax.axis_index("dp")
    count = width // chunk
    moves = [pltpu.make_async_copy(gt_v, gt_hbm, sem.at[0])]
    moves[0].start()
    wg_v[...] = jnp.dot(bt_v[pl.ds(pl.multiple_of(me * shard, 8), shard), :], q_v[...],
                        preferred_element_type=F32)
    moves.append(pltpu.make_async_copy(wg_v, wg_hbm.at[0], sem.at[1]))
    moves[1].start()
    for c in range(count):
        rows = pl.ds(c * chunk, chunk)
        low = jnp.dot(bt_v[rows, :], q_v[...], preferred_element_type=F32)
        err_v[rows, :] = (merged[rows, :] - low).astype(BF16)
        moves.append(pltpu.make_async_copy(err_v.at[rows], err_hbm.at[0, 0, rows], sem.at[2 + c]))
        moves[-1].start()
    for move in moves:
        move.wait()


def body(tokens, routes, gates, grad_hidden, w_in, error, q_seed):
    E = lax.axis_size("expert")
    N = lax.axis_size("dp")
    rows, width = tokens.shape
    hidden = grad_hidden.shape[2]
    rank = q_seed.shape[2]
    shard = width // N
    gather_w = shard % 16 == 0 and N & (N - 1) == 0
    weight = w_in[0] if gather_w else lax.all_gather(w_in[0], "dp", axis=0, tiled=True)
    chunk = 256 if width % 256 == 0 else 128
    C, CB = (4, 8) if E <= 8 else (2, 2)
    room = (4 * E + 3) * rows * width * 2 + 3 * E * rows * hidden * 2 + 13 * width * hidden + (12 << 20)
    total_rows = width // 128 * rank
    rp = -(-total_rows // N)
    rp = -(-rp // 16) * 16
    dma = pltpu.SemaphoreType.DMA
    vmem = pl.BlockSpec(memory_space=pltpu.VMEM)
    hbm = pl.BlockSpec(memory_space=pltpu.HBM)
    parts = pl.pallas_call(
        functools.partial(kernel, (E, N, rp, chunk, gather_w, C, CB)),
        out_shape=(
            jax.ShapeDtypeStruct((rows, width), BF16),
            jax.ShapeDtypeStruct((width, hidden), F32),
            jax.ShapeDtypeStruct((width, rank), BF16),
            jax.ShapeDtypeStruct((rank, hidden), BF16),
        ),
        in_specs=[hbm] * 7,
        out_specs=(vmem,) * 4,
        scratch_shapes=[
            pltpu.VMEM((E, rows, width), BF16),
            pltpu.VMEM((rows, 2, hidden), BF16),
            pltpu.VMEM((E, rows, hidden), BF16),
            pltpu.VMEM((E, rows, hidden), BF16),
            pltpu.VMEM((2, rows), jnp.int32),
            pltpu.VMEM((2, rows), F32),
            pltpu.VMEM((E, 8, rows), F32),
            pltpu.VMEM((E, 8, rows), F32),
            pltpu.VMEM((width, hidden), BF16),
            pltpu.VMEM((E, rows, width), BF16),
            pltpu.VMEM((E, rows, hidden), BF16),
            pltpu.VMEM((width, hidden), BF16),
            pltpu.VMEM((width, hidden), BF16),
            pltpu.VMEM((E, rows, width), BF16),
            pltpu.VMEM((E + 1, rows, width), BF16),
            pltpu.VMEM((rank, hidden), F32),
            pltpu.VMEM((2 * rank, hidden), BF16),
            pltpu.VMEM((rank, width), F32),
            pltpu.VMEM((rp * N, 128), BF16),
            pltpu.VMEM((N, rp, 128), BF16),
            pltpu.VMEM((rp * N, 128), BF16),
            pltpu.VMEM((N, rank, hidden), BF16),
            pltpu.SemaphoreType.REGULAR((2,)), dma((7,)), dma((2, E)), dma((E, C)), dma(()), dma((E,)), dma(()), dma((E,)),
            dma(()), dma((N,)), dma(()), dma(()), dma(()), dma(()), dma(()), dma(()),
            dma(()), dma((E,)), dma((E + 1, CB)),
        ],
        compiler_params=pltpu.CompilerParams(
            collective_id=0, has_side_effects=True, vmem_limit_bytes=min(room, 67043328 - (1 << 20))),
    )(*(pltpu.with_memory_space_constraint(a, pltpu.HBM) for a in (
        tokens, grad_hidden, routes.T, gates.T, weight, error, q_seed[0].T)))
    return pl.pallas_call(
        functools.partial(finish, chunk),
        out_shape=(
            jax.ShapeDtypeStruct((rows, width), BF16),
            jax.ShapeDtypeStruct((1, 1, width, hidden), BF16),
            jax.ShapeDtypeStruct((1, shard, hidden), F32),
        ),
        in_specs=[vmem] * 4,
        out_specs=(hbm, hbm, hbm),
        scratch_shapes=[
            pltpu.VMEM((width, hidden), BF16),
            pltpu.VMEM((shard, hidden), F32),
            dma((2 + width // chunk,)),
        ],
        compiler_params=pltpu.CompilerParams(vmem_limit_bytes=16 << 20),
    )(*parts)


def solution(mesh):
    placed = (
        P(("dp", "expert"), None),
        P(("dp", "expert"), None),
        P(("dp", "expert"), None),
        P(("dp", "expert"), None, None),
        P("expert", "dp", None),
        P("dp", "expert", None, None),
        P("expert", None, None),
    )
    return jax.shard_map(
        body,
        mesh=mesh,
        in_specs=placed,
        out_specs=(
            P(("dp", "expert"), None),
            P("dp", "expert", None, None),
            P("expert", "dp", None),
        ),
        check_vma=False,
    )
```
